32 devices in a mesh: gx: 4 (over z), gy: 2 (over y), gz: 4 (over x, core).
Axes of the slice: x: 2, y: 2, z: 4, core: 2. Of those that a mesh axis runs over, the one named last changes fastest.
Arguments:
- blocks: bfloat16 [8, 2, 8, 27, 128, 128], P('gx', 'gy', 'gz')
- pattern: int32 [8, 2, 8, 27], P('gx', 'gy'), may hold values 0 or 1
- order: int32 [8, 2, 8], P('gx', 'gy'), may hold values from 0 to 7, each once within a row
- start: float32 [8, 2, 8, 128], P('gx', 'gy', 'gz'), may hold values from -6 to 6
- rhs: float32 [8, 2, 8, 128], P('gx', 'gy', 'gz'), may hold values from -6 to 6
Outputs:
- smoothed: float32 [8, 2, 8, 128], P('gx', 'gy', 'gz')
- remainder: float32 [8, 2, 8, 128], P('gx', 'gy', 'gz')
The draws below stay inside these ranges and needn't reach their ends.
Inputs may be any that keep to these rules, and one draw needn't show every extreme that they name: `order`: in every grid column the 8 slots name each plane exactly once. `pattern`: entry 13 is ignored.
All inputs are finite; a program needn't handle non-finite values. No bound on the sum of `pattern` on one device may be relied on, other than what follows from the above.
Results may differ from the reference program's by a relative error of at most 0.0081.
Values may be sent and summed in bfloat16 or wider, within the bound.
No kernel may reach another device: no remote copies, remote signals or barrier semaphores. Data moves between devices by JAX's collectives and lax.ppermute only.
A program may use at most 64 MiB of HBM per device.

```python
import jax
import jax.numpy as jnp
from jax import lax

BS = 128
STENCIL = 27
DEG = 4
NX = 8
NY = 2
NZ = 8


def draw_blocks(key, part):
    shape = (NX, NY, NZ, STENCIL, BS, BS)
    spread = 0.7 / (STENCIL * BS) ** 0.5
    values = jax.random.normal(key, shape, jnp.float32) * spread
    values = values.at[:, :, :, 13].add(jnp.eye(BS, dtype=jnp.float32))
    return values.astype(jnp.bfloat16)


def place_ends(values, rng, smallest, largest):
    spot = [jax.random.randint(jax.random.fold_in(rng, axis), (), 0, length) for axis, length in enumerate(values.shape)]
    widest = values.shape.index(max(values.shape))
    next_to = spot[:widest] + [(spot[widest] + 1) % values.shape[widest]] + spot[widest + 1:]
    return values.at[tuple(spot)].set(smallest).at[tuple(next_to)].set(largest)


def steps_of(key, shape, split, least, largest):
    level = 1.0
    for dim, shards_of in split:
        heights = jax.random.uniform(jax.random.fold_in(jax.random.fold_in(key, 6), dim), (shards_of,), jnp.float32, least / len(split), largest / len(split))
        level = level * jnp.repeat(jnp.exp(heights), shape[dim] // shards_of).reshape((-1,) + (1,) * (len(shape) - 1 - dim))
    return level


def noise(stream_key, shape, scale, reach, shards=(), held_as=jnp.bfloat16):
    values = scale * jax.random.normal(stream_key, shape, jnp.float32)
    if shards:
        values = values * steps_of(stream_key, shape, shards, -0.22, 0.18)
    return jnp.clip(values, -reach, reach).astype(held_as)


def setup_inputs(seed: int = 0) -> dict:
    arg_keys = jax.random.split(jax.random.key(seed), 6)
    blocks = draw_blocks(jax.random.fold_in(arg_keys[5], 71), 0)
    pattern = place_ends((jax.random.randint(arg_keys[1], (NX, NY, NZ, STENCIL), 0, 4) < 3).astype(jnp.int32), jax.random.fold_in(arg_keys[1], 1), 0, 1)
    order = jax.vmap(lambda own: jax.random.permutation(own, NZ))(jax.random.split(arg_keys[2], NX * NY)).reshape((NX, NY, NZ)).astype(jnp.int32)
    start = noise(arg_keys[3], (NX, NY, NZ, BS), 1.0, 6.0, ((0, 4), (1, 2), (2, 4)), jnp.float32)
    rhs = noise(arg_keys[4], (NX, NY, NZ, BS), 1.0, 6.0, ((0, 4), (1, 2), (2, 4)), jnp.float32)
    return dict(blocks=blocks, pattern=pattern, order=order, start=start, rhs=rhs)


def coupled_values(vector, order, pattern):
    inverse = jnp.argsort(order, axis=2).astype(jnp.int32)
    rounded = vector.astype(jnp.bfloat16).astype(jnp.float32)
    planes = jnp.take_along_axis(rounded, jnp.broadcast_to(inverse[..., None], rounded.shape), axis=2)
    padded = jnp.pad(planes, ((1, 1), (1, 1), (1, 1), (0, 0)))
    span_x, span_y, span_z, width = vector.shape
    pieces = []
    for step_a in range(3):
        for step_b in range(3):
            column = padded[step_a:step_a + span_x, step_b:step_b + span_y]
            for step_c in range(3):
                index = jnp.broadcast_to((order + step_c)[..., None], (span_x, span_y, span_z, width)).astype(jnp.int32)
                pieces.append(jnp.take_along_axis(column, index, axis=2))
    gathered = jnp.stack(pieces, axis=3)
    present = jnp.where(jnp.arange(27) == 13, 1, pattern).astype(jnp.float32)
    return gathered * present[..., None]


def apply_operator(blocks, vector, order, pattern):
    gathered = coupled_values(vector, order, pattern)

    def one_plane(pair):
        values, matrix = pair
        return jnp.einsum("ysoj,ysoij->ysi", values, matrix.astype(jnp.float32))

    return lax.map(one_plane, (gathered, blocks))


def reference(blocks, pattern, order, start, rhs):
    center = 1.0
    spread = 0.8
    sigma = center / spread
    rho = 1.0 / sigma
    smoothed = start
    remainder = rhs - apply_operator(blocks, smoothed, order, pattern)
    search = remainder / center
    for number in range(DEG):
        smoothed = smoothed + search
        remainder = remainder - apply_operator(blocks, search, order, pattern)
        if number + 1 < DEG:
            following = 1.0 / (2.0 * sigma - rho)
            search = following * rho * search + (2.0 * following / spread) * remainder
            rho = following
    return smoothed, remainder
```

```python
import functools

import jax
import jax.numpy as jnp
from jax import lax
from jax.experimental import pallas as pl
from jax.experimental.pallas import tpu as pltpu
from jax.sharding import PartitionSpec as P

DEG = 4
CENTER = 1.0
SPREAD = 0.8
LANES = 128
GRANT = 16 * 2**20
AXES = ("gx", "gy", "gz")
VMEM = pl.BlockSpec(memory_space=pltpu.VMEM)
SMEM = pl.BlockSpec(memory_space=pltpu.SMEM)


def split(value, count):
    if count & (count - 1) == 0:
        shift = count.bit_length() - 1
        return value >> shift, value & (count - 1)
    whole = jnp.floor((value.astype(jnp.float32) + 0.5) * (1.0 / count)).astype(jnp.int32)
    return whole, value - whole * count


class Plan:
    def __init__(self, axis_sizes, local_shape):
        self.gx, self.gy, self.gz = axis_sizes
        self.nx, self.ny, self.nz, self.width = local_shape
        self.devices = self.gx * self.gy * self.gz
        self.rows = self.nx * self.ny * self.nz
        self.sent = 2 * self.rows
        self.sources = self.devices * self.sent
        self.few = self.ny == 1 and self.gy <= 2
        self.spans = min(3, self.gy) if self.few else 3
        self.entries = 9 * self.spans
        self.pitch = 32
        self.targets = -(-self.rows * self.pitch // LANES) * LANES

    def first_span(self):
        if not self.few:
            return 0
        return 1 - lax.axis_index("gy")

    def offsets(self, entry):
        return entry // (3 * self.spans), entry // 3 % self.spans, entry % 3

    def place(self, row):
        return row // (self.ny * self.nz), row // self.nz % self.ny, row % self.nz


def send(plan, vector, tail, pay_ref):
    tile = jnp.concatenate([vector, tail], axis=0).astype(jnp.bfloat16)
    pay_ref[...] = jnp.broadcast_to(tile[None], pay_ref.shape)


def first_kernel(plan, order_ref, start_ref, pay_ref):
    first = lax.axis_index("gz") * plan.nz
    planes = []
    for row in range(plan.rows):
        x, y, s = plan.place(row)
        planes.append(jnp.full((1, plan.width), order_ref[x, y, first + s], jnp.int32))
    planes = jnp.concatenate(planes, axis=0).astype(jnp.float32)
    send(plan, start_ref[...], planes, pay_ref)


def selection(plan, received_ref, order_ref, pattern_ref, select_ref):
    first = lax.axis_index("gz") * plan.nz
    lane = lax.broadcasted_iota(jnp.int32, (1, plan.targets), 1)
    row, entry = split(lane, plan.pitch)
    a, rest = split(entry, 3 * plan.spans)
    b, c = split(rest, 3)
    b = b + plan.first_span()
    plane = jnp.zeros_like(lane)
    keep = jnp.zeros_like(lane)
    for number in range(plan.rows):
        x, y, s = plan.place(number)
        plane = jnp.where(row == number, order_ref[x, y, first + s], plane)
        present = pattern_ref[x, y, pl.ds(first + s, 1), :]
        for index in range(plan.entries):
            i, j, k = plan.offsets(index)
            here = lane == number * plan.pitch + index
            if (i, k) == (1, 1):
                value = jnp.where(j + plan.first_span() == 1, 1, 0)
            else:
                value = 0
            for span in range(3):
                entry_of = 9 * i + 3 * span + k
                flag = present[:, entry_of : entry_of + 1]
                if entry_of == 13:
                    flag = jnp.ones_like(flag)
                match = j + plan.first_span() == span
                keep = jnp.where(here & match, flag, keep)
    x, y, s = row, row, row
    xy, s = split(row, plan.nz)
    x, y = split(xy, plan.ny)
    want_x = lax.axis_index("gx") * plan.nx + x + a - 1
    want_y = lax.axis_index("gy") * plan.ny + y + b - 1
    want_z = plane + c - 1
    keep = jnp.where((keep > 0) & (entry < plan.entries) & (row < plan.rows), 1, 0)

    source = lax.broadcasted_iota(jnp.int32, (plan.sources, LANES), 0)
    device, rank = split(source, plan.sent)
    device_xy, _ = split(device, plan.gz)
    device_x, device_y = split(device_xy, plan.gy)
    rank_xy, _ = split(rank, plan.nz)
    rank_x, rank_y = split(rank_xy, plan.ny)
    has_x = device_x * plan.nx + rank_x
    has_y = device_y * plan.ny + rank_y
    values = received_ref[...].astype(jnp.float32)
    has_z = pltpu.roll(values, plan.sources - plan.rows, 0).astype(jnp.int32)
    for block in range(plan.targets // LANES):
        part = slice(block * LANES, (block + 1) * LANES)
        hit = (has_x == want_x[:, part]) & (has_y == want_y[:, part]) & (has_z[:, :LANES] == want_z[:, part])
        hit = hit & (rank < plan.rows) & (keep[:, part] > 0)
        table = jnp.where(hit, 1.0, 0.0)
        select_ref[part, :] = table.T.astype(jnp.bfloat16)


def product(plan, blocks_ref, received_ref, select_ref, gather_ref, result_ref):
    gather_ref[...] = jnp.dot(
        select_ref[...], received_ref[...], preferred_element_type=jnp.float32
    )
    span = plan.first_span()
    size = plan.width
    lane = lax.broadcasted_iota(jnp.int32, (size, size), 1)
    line = lax.broadcasted_iota(jnp.int32, (size, size), 0)
    for row in range(plan.rows):
        x, y, s = plan.place(row)
        total = jnp.zeros((size, size), jnp.float32)
        for entry in range(plan.entries):
            i, j, k = plan.offsets(entry)
            at = row * plan.pitch + entry
            block = blocks_ref[x, y, s, 9 * i + 3 * (j + span) + k].astype(jnp.float32)
            total = total + block * gather_ref[at : at + 1, :]
        sums = jnp.sum(total, axis=1, keepdims=True)
        line_sums = jnp.where(lane == line, sums, 0.0)
        result_ref[row : row + 1, :] = jnp.sum(line_sums, axis=0, keepdims=True)


def opening_kernel(
    plan, received_ref, blocks_ref, order_ref, pattern_ref, start_ref, rhs_ref,
    pay_ref, select_ref, smoothed_ref, remainder_ref, search_ref, gather_ref, result_ref,
):
    selection(plan, received_ref, order_ref, pattern_ref, select_ref)
    product(plan, blocks_ref, received_ref, select_ref, gather_ref, result_ref)
    remainder = rhs_ref[...] - result_ref[...]
    search = remainder / CENTER
    send(plan, search, jnp.zeros_like(search), pay_ref)
    remainder_ref[...] = remainder
    search_ref[...] = search
    smoothed_ref[...] = start_ref[...] + search


def turn_kernel(
    plan, factors, received_ref, blocks_ref, select_ref, smoothed_in, remainder_in, search_in,
    pay_ref, smoothed_ref, remainder_ref, search_ref, gather_ref, result_ref,
):
    product(plan, blocks_ref, received_ref, select_ref, gather_ref, result_ref)
    remainder = remainder_in[...] - result_ref[...]
    search = factors[0] * search_in[...] + factors[1] * remainder
    send(plan, search, jnp.zeros_like(search), pay_ref)
    remainder_ref[...] = remainder
    search_ref[...] = search
    smoothed_ref[...] = smoothed_in[...] + search


def closing_kernel(
    plan, received_ref, blocks_ref, select_ref, remainder_in,
    remainder_ref, gather_ref, result_ref,
):
    product(plan, blocks_ref, received_ref, select_ref, gather_ref, result_ref)
    remainder_ref[...] = remainder_in[...] - result_ref[...]


def local(blocks, pattern, order, start, rhs):
    plan = Plan([lax.axis_size(axis) for axis in AXES], start.shape)
    state = jax.ShapeDtypeStruct((plan.rows, plan.width), jnp.float32)
    pay = jax.ShapeDtypeStruct((plan.devices, plan.sent, plan.width), jnp.bfloat16)
    select = jax.ShapeDtypeStruct((plan.targets, plan.sources), jnp.bfloat16)
    scratch = [
        pltpu.VMEM((plan.targets, plan.width), jnp.float32),
        pltpu.VMEM((plan.rows, plan.width), jnp.float32),
    ]

    def call(kernel, ins, outs, scratch_shapes=()):
        return pl.pallas_call(
            kernel,
            in_specs=ins,
            out_specs=[VMEM] * len(outs),
            out_shape=outs,
            scratch_shapes=scratch_shapes,
            compiler_params=pltpu.CompilerParams(vmem_limit_bytes=GRANT),
        )

    def exchange(sent):
        got = lax.all_to_all(sent, AXES, 0, 0, tiled=True)
        return got.reshape(plan.sources, plan.width)

    flat_start = start.reshape(state.shape)
    flat_rhs = rhs.reshape(state.shape)
    (sent,) = call(functools.partial(first_kernel, plan), [SMEM, VMEM], [pay])(order, flat_start)
    sent, table, smoothed, remainder, search = call(
        functools.partial(opening_kernel, plan),
        [VMEM, VMEM, SMEM, VMEM, VMEM, VMEM],
        [pay, select, state, state, state],
        scratch,
    )(exchange(sent), blocks, order, pattern, flat_start, flat_rhs)
    sigma = CENTER / SPREAD
    rho = 1.0 / sigma
    for number in range(DEG - 1):
        following = 1.0 / (2.0 * sigma - rho)
        factors = (following * rho, 2.0 * following / SPREAD)
        rho = following
        sent, smoothed, remainder, search = call(
            functools.partial(turn_kernel, plan, factors),
            [VMEM] * 6,
            [pay, state, state, state],
            scratch,
        )(exchange(sent), blocks, table, smoothed, remainder, search)
    (remainder,) = call(
        functools.partial(closing_kernel, plan), [VMEM] * 4, [state], scratch
    )(exchange(sent), blocks, table, remainder)
    return smoothed.reshape(start.shape), remainder.reshape(start.shape)


def solution(mesh):
    in_specs = (
        P("gx", "gy", "gz", None, None, None),
        P("gx", "gy", None, None),
        P("gx", "gy", None),
        P("gx", "gy", "gz", None),
        P("gx", "gy", "gz", None),
    )
    out_specs = (P("gx", "gy", "gz", None), P("gx", "gy", "gz", None))
    return jax.shard_map(local, mesh=mesh, in_specs=in_specs, out_specs=out_specs, check_vma=False)
```

```python
import functools

import jax
import jax.numpy as jnp
from jax import lax
from jax.experimental import pallas as pl
from jax.experimental.pallas import tpu as pltpu
from jax.sharding import PartitionSpec as P

DEG = 4
CENTER = 1.0
SPREAD = 0.8
LANES = 128
PITCH = 32
GRANT = 16 * 2**20
AXES = ("gx", "gy", "gz")
VMEM = pl.BlockSpec(memory_space=pltpu.VMEM)
HBM = pl.BlockSpec(memory_space=pltpu.HBM)


def split(value, count):
    if count & (count - 1) == 0:
        shift = count.bit_length() - 1
        return value >> shift, value & (count - 1)
    whole = jnp.floor((value.astype(jnp.float32) + 0.5) * (1.0 / count)).astype(jnp.int32)
    return whole, value - whole * count


def far(array):
    return pltpu.with_memory_space_constraint(array, pltpu.HBM)


class Plan:
    def __init__(self, axis_sizes, local_shape):
        self.gx, self.gy, self.gz = axis_sizes
        self.nx, self.ny, self.nz, self.width = local_shape
        self.devices = self.gx * self.gy * self.gz
        self.rows = self.nx * self.ny * self.nz
        self.sources = self.devices * self.rows
        self.few = self.ny == 1 and self.gy <= 2
        self.spans = min(3, self.gy) if self.few else 3
        self.entries = [(i, j, k) for i in range(3) for j in range(self.spans) for k in range(3)]
        self.targets = -(-self.rows * PITCH // LANES) * LANES

    def first_span(self):
        return 1 - lax.axis_index("gy") if self.few else 0

    def place(self, row):
        return row // (self.ny * self.nz), row // self.nz % self.ny, row % self.nz

    def key(self, x, y, z):
        return ((x + 1) * (self.gy * self.ny + 2) + y + 1) * (self.gz * self.nz + 2) + z + 1


def send(tile, pay_ref):
    pay_ref[...] = jnp.broadcast_to(tile.astype(jnp.bfloat16)[None], pay_ref.shape)


def first_kernel(
    plan, order_hbm, pattern_hbm, start_hbm,
    pay_ref, want_ref, start_ref, order_ref, pattern_ref, sems,
):
    copies = (
        pltpu.make_async_copy(order_hbm, order_ref, sems.at[0]),
        pltpu.make_async_copy(pattern_hbm, pattern_ref, sems.at[1]),
        pltpu.make_async_copy(start_hbm, start_ref, sems.at[2]),
    )
    for copy in copies:
        copy.start()
    for copy in copies:
        copy.wait()
    first = lax.axis_index("gz") * plan.nz
    line = lax.broadcasted_iota(jnp.int32, (plan.rows, plan.width), 0)
    planes = jnp.zeros_like(line)
    for row in range(plan.rows):
        x, y, s = plan.place(row)
        planes = jnp.where(line == row, order_ref[x, y, first + s], planes)
    send(jnp.concatenate([start_ref[...], planes.astype(jnp.float32)], axis=0), pay_ref)
    want_ref[...] = wanted(plan, order_ref, pattern_ref)


def wanted(plan, order_ref, pattern_ref):
    first = lax.axis_index("gz") * plan.nz
    span = plan.first_span()
    lane = lax.broadcasted_iota(jnp.int32, (1, plan.targets), 1)
    row, entry = split(lane, PITCH)
    a = (entry * 57) >> 9
    rest = entry - 9 * a
    b = (rest * 43) >> 7
    c = rest - 3 * b
    plane = jnp.zeros_like(lane)
    keep = jnp.zeros_like(lane)
    for number in range(plan.rows):
        x, y, s = plan.place(number)
        plane = jnp.where(row == number, order_ref[x, y, first + s], plane)
        flags = pattern_ref[x, y, pl.ds(first + s, 1), :]
        gap = jnp.zeros((1, plan.targets - flags.shape[1]), jnp.int32)
        flags = jnp.concatenate([flags, gap], axis=1)
        keep = keep + (pltpu.roll(flags, PITCH * number, 1) if number else flags)
    if plan.few:
        keep = jnp.where(span == 1, pltpu.roll(keep, plan.targets - 3, 1), keep)
    b = b + span
    keep = ((keep > 0) | (9 * a + 3 * b + c == 13)) & (entry < 27) & (row < plan.rows)
    xy, _ = split(row, plan.nz)
    x, y = split(xy, plan.ny)
    x = lax.axis_index("gx") * plan.nx + x + a - 1
    y = lax.axis_index("gy") * plan.ny + y + b - 1
    return jnp.where(keep, plan.key(x, y, plane + c - 1), -1)


def held(plan, planes):
    source = lax.broadcasted_iota(jnp.int32, (plan.sources, LANES), 0)
    device, rank = split(source, plan.rows)
    device_xy, _ = split(device, plan.gz)
    device_x, device_y = split(device_xy, plan.gy)
    rank_xy, _ = split(rank, plan.nz)
    rank_x, rank_y = split(rank_xy, plan.ny)
    return plan.key(device_x * plan.nx + rank_x, device_y * plan.ny + rank_y, planes)


def selection(plan, planes, want, select_ref):
    have = held(plan, planes)
    for first in range(0, plan.targets, LANES):
        part = slice(first, first + LANES)
        table = jnp.where(have == want[:, part], 1.0, 0.0)
        select_ref[part, :] = table.T.astype(jnp.bfloat16)


def stage(plan, received_ref, stage_ref, first):
    for device in range(plan.devices):
        part = received_ref[device, first : first + plan.rows, :].astype(jnp.float32)
        stage_ref[device * plan.rows : (device + 1) * plan.rows, :] = part


def product(plan, blocks_ref, received_ref, select_ref, stage_ref, gather_ref, result_ref):
    stage(plan, received_ref, stage_ref, 0)
    gather_ref[...] = jnp.dot(
        select_ref[...], stage_ref[...].astype(jnp.bfloat16), preferred_element_type=jnp.float32
    )
    span = plan.first_span()
    size = plan.width
    lane = lax.broadcasted_iota(jnp.int32, (size, size), 1)
    line = lax.broadcasted_iota(jnp.int32, (size, size), 0)
    for row in range(plan.rows):
        x, y, s = plan.place(row)
        total = jnp.zeros((size, size), jnp.float32)
        for i, j, k in plan.entries:
            at = row * PITCH + 9 * i + 3 * j + k
            block = blocks_ref[x, y, s, 9 * i + 3 * (j + span) + k].astype(jnp.float32)
            total = total + block * gather_ref[at : at + 1, :]
        sums = jnp.sum(total, axis=1, keepdims=True)
        line_sums = jnp.where(lane == line, sums, 0.0)
        result_ref[row : row + 1, :] = jnp.sum(line_sums, axis=0, keepdims=True)


def opening_kernel(
    plan, received_ref, blocks_ref, want_ref, start_ref, rhs_ref,
    pay_ref, select_ref, smoothed_ref, remainder_ref, search_ref,
    stage_ref, gather_ref, result_ref,
):
    stage(plan, received_ref, stage_ref, plan.rows)
    planes = stage_ref[...].astype(jnp.int32)
    selection(plan, planes, want_ref[...], select_ref)
    product(plan, blocks_ref, received_ref, select_ref, stage_ref, gather_ref, result_ref)
    remainder = rhs_ref[...] - result_ref[...]
    search = remainder / CENTER
    send(search, pay_ref)
    remainder_ref[...] = remainder
    search_ref[...] = search
    smoothed_ref[...] = start_ref[...] + search


def turn_kernel(
    plan, factors, received_ref, blocks_ref, select_ref, smoothed_in, remainder_in, search_in,
    pay_ref, smoothed_ref, remainder_ref, search_ref,
    stage_ref, gather_ref, result_ref,
):
    product(plan, blocks_ref, received_ref, select_ref, stage_ref, gather_ref, result_ref)
    remainder = remainder_in[...] - result_ref[...]
    search = factors[0] * search_in[...] + factors[1] * remainder
    send(search, pay_ref)
    remainder_ref[...] = remainder
    search_ref[...] = search
    smoothed_ref[...] = smoothed_in[...] + search


def closing_kernel(
    plan, received_ref, blocks_ref, select_ref, smoothed_in, remainder_in,
    smoothed_ref, remainder_ref, stage_ref, gather_ref, result_ref,
):
    product(plan, blocks_ref, received_ref, select_ref, stage_ref, gather_ref, result_ref)
    remainder_ref[...] = remainder_in[...] - result_ref[...]
    smoothed_ref[...] = smoothed_in[...]


def local(blocks, pattern, order, start, rhs):
    plan = Plan([lax.axis_size(axis) for axis in AXES], start.shape)
    state = jax.ShapeDtypeStruct((plan.rows, plan.width), jnp.float32)
    select = jax.ShapeDtypeStruct((plan.targets, plan.sources), jnp.bfloat16)
    scratch = [
        pltpu.VMEM((plan.sources, plan.width), jnp.float32),
        pltpu.VMEM((plan.targets, plan.width), jnp.float32),
        pltpu.VMEM((plan.rows, plan.width), jnp.float32),
    ]

    def pay(rows):
        return jax.ShapeDtypeStruct((plan.devices, rows, plan.width), jnp.bfloat16)

    def call(kernel, ins, outs, scratch_shapes, cost=None):
        return pl.pallas_call(
            kernel,
            in_specs=ins,
            out_specs=[VMEM] * len(outs),
            out_shape=outs,
            scratch_shapes=scratch_shapes,
            compiler_params=pltpu.CompilerParams(vmem_limit_bytes=GRANT),
            cost_estimate=cost,
        )

    def exchange(sent):
        return lax.all_to_all(sent, AXES, 0, 0, tiled=True)

    flat_start = start.reshape(state.shape)
    flat_rhs = rhs.reshape(state.shape)
    sent, want = call(
        functools.partial(first_kernel, plan),
        [HBM, HBM, HBM],
        [pay(2 * plan.rows), jax.ShapeDtypeStruct((1, plan.targets), jnp.int32)],
        [
            pltpu.VMEM(state.shape, jnp.float32),
            pltpu.SMEM(order.shape, jnp.int32),
            pltpu.VMEM(pattern.shape, jnp.int32),
            pltpu.SemaphoreType.DMA((3,)),
        ],
        pl.CostEstimate(flops=10**10, bytes_accessed=10**8, transcendentals=0),
    )(far(order), far(pattern), far(flat_start))
    sent, table, smoothed, remainder, search = call(
        functools.partial(opening_kernel, plan),
        [VMEM] * 5,
        [pay(plan.rows), select, state, state, state],
        scratch,
    )(exchange(sent), blocks, want, flat_start, flat_rhs)
    sigma = CENTER / SPREAD
    rho = 1.0 / sigma
    for _ in range(DEG - 1):
        following = 1.0 / (2.0 * sigma - rho)
        factors = (following * rho, 2.0 * following / SPREAD)
        rho = following
        sent, smoothed, remainder, search = call(
            functools.partial(turn_kernel, plan, factors),
            [VMEM] * 6,
            [pay(plan.rows), state, state, state],
            scratch,
        )(exchange(sent), blocks, table, smoothed, remainder, search)
    smoothed, remainder = call(
        functools.partial(closing_kernel, plan), [VMEM] * 5, [state, state], scratch
    )(exchange(sent), blocks, table, smoothed, remainder)
    return smoothed.reshape(start.shape), remainder.reshape(start.shape)


def solution(mesh):
    in_specs = (
        P("gx", "gy", "gz", None, None, None),
        P("gx", "gy", None, None),
        P("gx", "gy", None),
        P("gx", "gy", "gz", None),
        P("gx", "gy", "gz", None),
    )
    out_specs = (P("gx", "gy", "gz", None), P("gx", "gy", "gz", None))
    return jax.shard_map(local, mesh=mesh, in_specs=in_specs, out_specs=out_specs, check_vma=False)
```

```python
import functools

import jax
import jax.numpy as jnp
from jax import lax
from jax.experimental import pallas as pl
from jax.experimental.pallas import tpu as pltpu
from jax.sharding import PartitionSpec as P

DEG = 4
CENTER = 1.0
SPREAD = 0.8
LANES = 128
PITCH = 32
GRANT = 16 * 2**20
AXES = ("gz", "gx", "gy")
VMEM = pl.BlockSpec(memory_space=pltpu.VMEM)
HBM = pl.BlockSpec(memory_space=pltpu.HBM)


def split(value, count):
    if count & (count - 1) == 0:
        shift = count.bit_length() - 1
        return value >> shift, value & (count - 1)
    whole = jnp.floor((value.astype(jnp.float32) + 0.5) * (1.0 / count)).astype(jnp.int32)
    return whole, value - whole * count


def far(array):
    return pltpu.with_memory_space_constraint(array, pltpu.HBM)


class Rounded:
    def __init__(self, ref):
        self.ref = ref

    def __getitem__(self, index):
        return self.ref[index].astype(jnp.bfloat16)


class Plan:
    def __init__(self, axis_sizes, local_shape):
        self.gx, self.gy, self.gz = axis_sizes
        self.nx, self.ny, self.nz, self.width = local_shape
        self.devices = self.gx * self.gy * self.gz
        self.rows = self.nx * self.ny * self.nz
        self.sources = self.devices * self.rows
        self.few = self.ny == 1 and self.gy <= 2
        self.spans = min(3, self.gy) if self.few else 3
        self.entries = [(i, j, k) for i in range(3) for j in range(self.spans) for k in range(3)]
        self.targets = -(-self.rows * PITCH // LANES) * LANES
        self.lot = -(-self.rows // 8) * 8
        self.half = -(-(len(self.entries) + 1) // 2 * self.lot // 16) * 16

    def first_span(self):
        return 1 - lax.axis_index("gy") if self.few else 0

    def place(self, row):
        return row // (self.ny * self.nz), row // self.nz % self.ny, row % self.nz

    def spot(self, number):
        return number % 2 * self.half + number // 2 * self.lot

    def key(self, x, y, z):
        return ((x + 1) * (self.gy * self.ny + 2) + y + 1) * (self.gz * self.nz + 2) + z + 1


def send(tile, pay_ref):
    pay_ref[...] = jnp.broadcast_to(tile.astype(jnp.bfloat16)[None], pay_ref.shape)


def first_kernel(
    plan, order_hbm, pattern_hbm, start_hbm,
    pay_ref, want_ref, start_ref, order_ref, pattern_ref, sems,
):
    copies = (
        pltpu.make_async_copy(order_hbm, order_ref, sems.at[0]),
        pltpu.make_async_copy(pattern_hbm, pattern_ref, sems.at[1]),
        pltpu.make_async_copy(start_hbm, start_ref, sems.at[2]),
    )
    for copy in copies:
        copy.start()
    for copy in copies:
        copy.wait()
    first = lax.axis_index("gz") * plan.nz
    line = lax.broadcasted_iota(jnp.int32, (plan.rows, plan.width), 0)
    planes = jnp.zeros_like(line)
    for row in range(plan.rows):
        x, y, s = plan.place(row)
        planes = jnp.where(line == row, order_ref[x, y, first + s], planes)
    send(jnp.concatenate([start_ref[...], planes.astype(jnp.float32)], axis=0), pay_ref)
    want_ref[...] = wanted(plan, order_ref, pattern_ref)


def wanted(plan, order_ref, pattern_ref):
    first = lax.axis_index("gz") * plan.nz
    span = plan.first_span()
    lane = lax.broadcasted_iota(jnp.int32, (1, plan.targets), 1)
    row, entry = split(lane, PITCH)
    a = (entry * 57) >> 9
    rest = entry - 9 * a
    b = (rest * 43) >> 7
    c = rest - 3 * b
    plane = jnp.zeros_like(lane)
    keep = jnp.zeros_like(lane)
    for number in range(plan.rows):
        x, y, s = plan.place(number)
        plane = jnp.where(row == number, order_ref[x, y, first + s], plane)
        flags = pattern_ref[x, y, pl.ds(first + s, 1), :]
        gap = jnp.zeros((1, plan.targets - flags.shape[1]), jnp.int32)
        flags = jnp.concatenate([flags, gap], axis=1)
        keep = keep + (pltpu.roll(flags, PITCH * number, 1) if number else flags)
    if plan.few:
        keep = jnp.where(span == 1, pltpu.roll(keep, plan.targets - 3, 1), keep)
    b = b + span
    keep = ((keep > 0) | (9 * a + 3 * b + c == 13)) & (entry < 27) & (row < plan.rows)
    xy, _ = split(row, plan.nz)
    x, y = split(xy, plan.ny)
    x = lax.axis_index("gx") * plan.nx + x + a - 1
    y = lax.axis_index("gy") * plan.ny + y + b - 1
    return jnp.where(keep, plan.key(x, y, plane + c - 1), -1)


def held(plan, planes):
    source = lax.broadcasted_iota(jnp.int32, (plan.sources, LANES), 0)
    device, rank = split(source, plan.rows)
    _, device_xy = split(device, plan.gx * plan.gy)
    device_x, device_y = split(device_xy, plan.gy)
    rank_xy, _ = split(rank, plan.nz)
    rank_x, rank_y = split(rank_xy, plan.ny)
    return plan.key(device_x * plan.nx + rank_x, device_y * plan.ny + rank_y, planes)


def selection(plan, planes, want, table_ref, wide_ref, select_ref):
    have = held(plan, planes)
    wide_ref[...] = jnp.zeros_like(wide_ref)
    for begin in range(0, plan.sources, LANES):
        some = slice(begin, begin + LANES)
        for first in range(0, plan.targets, LANES):
            part = slice(first, first + LANES)
            table_ref[part, :] = jnp.where(have[some] == want[:, part], 1.0, 0.0).T
        for number, (i, j, k) in enumerate(plan.entries):
            rows = table_ref[pl.ds(9 * i + 3 * j + k, plan.rows, stride=PITCH), :]
            at = plan.spot(number)
            wide_ref[at : at + plan.rows, some] = rows
    select_ref[...] = wide_ref[...].astype(jnp.bfloat16)


def product(plan, blocks_ref, rows_ref, select_ref, gather_ref):
    gather_ref[...] = jnp.dot(select_ref[...], rows_ref[...], preferred_element_type=jnp.float32)
    span = plan.first_span()
    size = plan.width

    def block(row, number):
        x, y, s = plan.place(row)
        i, j, k = plan.entries[number]
        return blocks_ref[x, y, s, 9 * i + 3 * (j + span) + k]

    results = [None] * plan.rows
    count = len(plan.entries) // 2
    for low in range(0, plan.rows // 4 * 2, 2):
        sums = []
        for part in (range(0, count // 2), range(count // 2, count)):
            left, right = [], []
            for pair in part:
                for side in (0, 1):
                    at = plan.spot(2 * pair + side)
                    left.append(gather_ref[at : at + plan.lot, :].astype(jnp.bfloat16))
                    right.append(
                        jnp.concatenate([block(row, 2 * pair + side) for row in (low, low + 1)], axis=0)
                    )
            sums.append(
                lax.dot_general(
                    jnp.concatenate(left, axis=1),
                    jnp.concatenate(right, axis=1),
                    (((1,), (1,)), ((), ())),
                    preferred_element_type=jnp.float32,
                )
            )
        both = sums[0] + sums[1]
        results[low] = both[low : low + 1, :size]
        results[low + 1] = both[low + 1 : low + 2, size:]

    lane = lax.broadcasted_iota(jnp.int32, (size, size), 1)
    line = lax.broadcasted_iota(jnp.int32, (size, size), 0)
    for row in range(plan.rows):
        if results[row] is None:
            numbers = range(len(plan.entries))
        else:
            numbers = range(2 * count, len(plan.entries))
        if not numbers:
            continue
        total = jnp.zeros((size, size), jnp.float32)
        for number in numbers:
            at = plan.spot(number) + row
            total = total + block(row, number).astype(jnp.float32) * gather_ref[at : at + 1, :]
        sums = jnp.sum(total, axis=1, keepdims=True)
        found = jnp.sum(jnp.where(lane == line, sums, 0.0), axis=0, keepdims=True)
        results[row] = found if results[row] is None else results[row] + found
    return jnp.concatenate(results, axis=0)


def opening_kernel(
    plan, received_ref, blocks_ref, want_ref, start_ref, rhs_ref,
    pay_ref, select_ref, smoothed_ref, remainder_ref, search_ref,
    gather_ref, stage_ref, rows_ref, table_ref, wide_ref,
):
    for device in range(plan.devices):
        here = slice(device * plan.rows, (device + 1) * plan.rows)
        values = received_ref[device].astype(jnp.float32)
        rows_ref[here, :] = values[: plan.rows]
        stage_ref[here, :] = values[plan.rows :]
    selection(plan, stage_ref[...].astype(jnp.int32), want_ref[...], table_ref, wide_ref, select_ref)
    remainder = rhs_ref[...] - product(
        plan, blocks_ref, Rounded(rows_ref), select_ref, gather_ref
    )
    search = remainder / CENTER
    send(search, pay_ref)
    remainder_ref[...] = remainder
    search_ref[...] = search
    smoothed_ref[...] = start_ref[...] + search


def turn_kernel(
    plan, factors, received_ref, blocks_ref, select_ref, smoothed_in, remainder_in, search_in,
    pay_ref, smoothed_ref, remainder_ref, *rest,
):
    *search_ref, gather_ref = rest
    remainder = remainder_in[...] - product(plan, blocks_ref, received_ref, select_ref, gather_ref)
    search = factors[0] * search_in[...] + factors[1] * remainder
    send(search, pay_ref)
    remainder_ref[...] = remainder
    smoothed_ref[...] = smoothed_in[...] + search
    if search_ref:
        search_ref[0][...] = search


def closing_kernel(
    plan, received_ref, blocks_ref, select_ref, smoothed_in, remainder_in,
    smoothed_ref, remainder_ref, gather_ref,
):
    smoothed_ref[...] = smoothed_in[...]
    remainder_ref[...] = remainder_in[...] - product(
        plan, blocks_ref, received_ref, select_ref, gather_ref
    )


def local(blocks, pattern, order, start, rhs):
    plan = Plan([lax.axis_size(axis) for axis in ("gx", "gy", "gz")], start.shape)
    state = jax.ShapeDtypeStruct((plan.rows, plan.width), jnp.float32)
    select = jax.ShapeDtypeStruct((2 * plan.half, plan.sources), jnp.bfloat16)
    gather = [pltpu.VMEM((2 * plan.half, plan.width), jnp.float32)]
    tables = [
        pltpu.VMEM((plan.sources, plan.width), jnp.float32),
        pltpu.VMEM((plan.sources, plan.width), jnp.float32),
        pltpu.VMEM((plan.targets, LANES), jnp.float32),
        pltpu.VMEM((2 * plan.half, plan.sources), jnp.float32),
    ]

    def pay(rows):
        return jax.ShapeDtypeStruct((plan.devices, rows, plan.width), jnp.bfloat16)

    def call(kernel, ins, outs, scratch_shapes, cost=None):
        return pl.pallas_call(
            kernel,
            in_specs=ins,
            out_specs=[VMEM] * len(outs),
            out_shape=outs,
            scratch_shapes=scratch_shapes,
            compiler_params=pltpu.CompilerParams(vmem_limit_bytes=GRANT),
            cost_estimate=cost,
        )

    def exchange(sent):
        return lax.all_to_all(sent, AXES, 0, 0, tiled=True)

    def packed(received):
        return received.reshape(plan.sources, plan.width)

    flat_start = start.reshape(state.shape)
    flat_rhs = rhs.reshape(state.shape)
    sent, want = call(
        functools.partial(first_kernel, plan),
        [HBM, HBM, HBM],
        [pay(2 * plan.rows), jax.ShapeDtypeStruct((1, plan.targets), jnp.int32)],
        [
            pltpu.VMEM(state.shape, jnp.float32),
            pltpu.SMEM(order.shape, jnp.int32),
            pltpu.VMEM(pattern.shape, jnp.int32),
            pltpu.SemaphoreType.DMA((3,)),
        ],
        pl.CostEstimate(flops=10**10, bytes_accessed=10**8, transcendentals=0),
    )(far(order), far(pattern), far(flat_start))
    sent, table, smoothed, remainder, search = call(
        functools.partial(opening_kernel, plan),
        [VMEM] * 5,
        [pay(plan.rows), select, state, state, state],
        gather + tables,
    )(exchange(sent), blocks, want, flat_start, flat_rhs)
    sigma = CENTER / SPREAD
    rho = 1.0 / sigma
    search = [search]
    for number in range(DEG - 1):
        following = 1.0 / (2.0 * sigma - rho)
        factors = (following * rho, 2.0 * following / SPREAD)
        rho = following
        states = [state] * (3 if number + 2 < DEG else 2)
        sent, smoothed, remainder, *search = call(
            functools.partial(turn_kernel, plan, factors),
            [VMEM] * 6,
            [pay(plan.rows)] + states,
            gather,
        )(packed(exchange(sent)), blocks, table, smoothed, remainder, *search)
    smoothed, remainder = call(
        functools.partial(closing_kernel, plan), [VMEM] * 5, [state, state], gather
    )(packed(exchange(sent)), blocks, table, smoothed, remainder)
    return smoothed.reshape(start.shape), remainder.reshape(start.shape)


def solution(mesh):
    in_specs = (
        P("gx", "gy", "gz", None, None, None),
        P("gx", "gy", None, None),
        P("gx", "gy", None),
        P("gx", "gy", "gz", None),
        P("gx", "gy", "gz", None),
    )
    out_specs = (P("gx", "gy", "gz", None), P("gx", "gy", "gz", None))
    return jax.shard_map(local, mesh=mesh, in_specs=in_specs, out_specs=out_specs, check_vma=False)
```

```python
import functools

import jax
import jax.numpy as jnp
from jax import lax
from jax.experimental import pallas as pl
from jax.experimental.pallas import tpu as pltpu
from jax.sharding import PartitionSpec as P

DEG = 4
CENTER = 1.0
SPREAD = 0.8
LANES = 128
PITCH = 32
GRANT = 16 * 2**20
AXES = ("gz", "gx", "gy")
VMEM = pl.BlockSpec(memory_space=pltpu.VMEM)
HBM = pl.BlockSpec(memory_space=pltpu.HBM)


def split(value, count):
    if count & (count - 1) == 0:
        shift = count.bit_length() - 1
        return value >> shift, value & (count - 1)
    whole = jnp.floor((value.astype(jnp.float32) + 0.5) * (1.0 / count)).astype(jnp.int32)
    return whole, value - whole * count


def far(array):
    return pltpu.with_memory_space_constraint(array, pltpu.HBM)


class Rounded:
    def __init__(self, ref):
        self.ref = ref

    def __getitem__(self, index):
        return self.ref[index].astype(jnp.bfloat16)


class Plan:
    def __init__(self, axis_sizes, local_shape):
        self.gx, self.gy, self.gz = axis_sizes
        self.nx, self.ny, self.nz, self.width = local_shape
        self.devices = self.gx * self.gy * self.gz
        self.rows = self.nx * self.ny * self.nz
        self.sources = self.devices * self.rows
        self.few = self.ny == 1 and self.gy <= 2
        self.spans = min(3, self.gy) if self.few else 3
        self.entries = [(i, j, k) for i in range(3) for j in range(self.spans) for k in range(3)]
        self.targets = -(-self.rows * PITCH // LANES) * LANES
        self.tiled = list(range(self.rows // 4))
        self.plain = list(range(self.rows // 4, self.rows))
        self.quads = -(-len(self.entries) // 4)
        self.half = 8 * self.quads * len(self.tiled)
        lines = 2 * self.half + len(self.plain) * len(self.entries)
        self.lines = -(-lines // 16) * 16

    def first_span(self):
        return 1 - lax.axis_index("gy") if self.few else 0

    def place(self, row):
        return row // (self.ny * self.nz), row // self.nz % self.ny, row % self.nz

    def lot(self, row, quad, side):
        return side * self.half + 8 * (row * self.quads + quad)

    def spot(self, row, number):
        if row in self.tiled:
            return self.lot(row, number // 4, number % 2) + number % 4 // 2
        return 2 * self.half + (row - len(self.tiled)) * len(self.entries) + number

    def key(self, x, y, z):
        return ((x + 1) * (self.gy * self.ny + 2) + y + 1) * (self.gz * self.nz + 2) + z + 1


def send(tile, pay_ref):
    pay_ref[...] = jnp.broadcast_to(tile.astype(jnp.bfloat16)[None], pay_ref.shape)


def first_kernel(
    plan, order_hbm, pattern_hbm, start_hbm,
    pay_ref, want_ref, start_ref, order_ref, pattern_ref, sems,
):
    copies = (
        pltpu.make_async_copy(order_hbm, order_ref, sems.at[0]),
        pltpu.make_async_copy(pattern_hbm, pattern_ref, sems.at[1]),
        pltpu.make_async_copy(start_hbm, start_ref, sems.at[2]),
    )
    for copy in copies:
        copy.start()
    for copy in copies:
        copy.wait()
    first = lax.axis_index("gz") * plan.nz
    line = lax.broadcasted_iota(jnp.int32, (plan.rows, plan.width), 0)
    planes = jnp.zeros_like(line)
    for row in range(plan.rows):
        x, y, s = plan.place(row)
        planes = jnp.where(line == row, order_ref[x, y, first + s], planes)
    send(jnp.concatenate([start_ref[...], planes.astype(jnp.float32)], axis=0), pay_ref)
    want_ref[...] = wanted(plan, order_ref, pattern_ref)


def wanted(plan, order_ref, pattern_ref):
    first = lax.axis_index("gz") * plan.nz
    span = plan.first_span()
    lane = lax.broadcasted_iota(jnp.int32, (1, plan.targets), 1)
    row, entry = split(lane, PITCH)
    a = (entry * 57) >> 9
    rest = entry - 9 * a
    b = (rest * 43) >> 7
    c = rest - 3 * b
    plane = jnp.zeros_like(lane)
    keep = jnp.zeros_like(lane)
    for number in range(plan.rows):
        x, y, s = plan.place(number)
        plane = jnp.where(row == number, order_ref[x, y, first + s], plane)
        flags = pattern_ref[x, y, pl.ds(first + s, 1), :]
        gap = jnp.zeros((1, plan.targets - flags.shape[1]), jnp.int32)
        flags = jnp.concatenate([flags, gap], axis=1)
        keep = keep + pltpu.roll(flags, lax.rem(plan.targets + PITCH * number - 3 * span, plan.targets), 1)
    b = b + span
    keep = ((keep > 0) | (9 * a + 3 * b + c == 13)) & (entry < 27) & (row < plan.rows)
    xy, _ = split(row, plan.nz)
    x, y = split(xy, plan.ny)
    x = lax.axis_index("gx") * plan.nx + x + a - 1
    y = lax.axis_index("gy") * plan.ny + y + b - 1
    return jnp.where(keep, plan.key(x, y, plane + c - 1), -1)


def held(plan, planes):
    source = lax.broadcasted_iota(jnp.int32, (plan.sources, LANES), 0)
    device, rank = split(source, plan.rows)
    _, device_xy = split(device, plan.gx * plan.gy)
    device_x, device_y = split(device_xy, plan.gy)
    rank_xy, _ = split(rank, plan.nz)
    rank_x, rank_y = split(rank_xy, plan.ny)
    return plan.key(device_x * plan.nx + rank_x, device_y * plan.ny + rank_y, planes)


def selection(plan, planes, want, table_ref, wide_ref, select_ref):
    have = held(plan, planes)
    wide_ref[...] = jnp.zeros_like(wide_ref)
    for begin in range(0, plan.sources, LANES):
        some = slice(begin, begin + LANES)
        for first in range(0, plan.targets, LANES):
            part = slice(first, first + LANES)
            table_ref[part, :] = jnp.where(have[some] == want[:, part], 1.0, 0.0).T
        for row in range(plan.rows):
            for number, (i, j, k) in enumerate(plan.entries):
                line = PITCH * row + 9 * i + 3 * j + k
                at = plan.spot(row, number)
                wide_ref[at : at + 1, some] = table_ref[line : line + 1, :]
    select_ref[...] = wide_ref[...].astype(jnp.bfloat16)


def product(plan, blocks_ref, wide_ref, rows_ref, select_ref, gather_ref, opening=False):
    gather_ref[...] = jnp.dot(select_ref[...], rows_ref[...], preferred_element_type=jnp.float32)
    span = plan.first_span()
    size = plan.width
    count = len(plan.entries)

    def block(row, number):
        x, y, s = plan.place(row)
        i, j, k = plan.entries[number]
        return blocks_ref[x, y, s, 9 * i + 3 * (j + span) + k]

    def pair(row, number):
        blank = jnp.zeros((size, size), jnp.bfloat16)
        sides = [block(row, at) if at < count else blank for at in (number, number + 1)]
        return jnp.concatenate(sides, axis=1)

    results = []
    for row in plan.tiled:
        found = jnp.zeros((1, size), jnp.float32)
        whole = [quad for quad in range(plan.quads) if 4 * quad + 2 < count]
        cut = len(whole) // 2
        for group in (whole[:cut], whole[cut:], [plan.quads - 1] if plan.quads > len(whole) else []):
            if not group:
                continue
            left, right = [], []
            for quad in group:
                for side in (0, 1):
                    at = plan.lot(row, quad, side)
                    left.append(gather_ref[at : at + 8, :].astype(jnp.bfloat16))
                parts = [pair(row, at) for at in (4 * quad, 4 * quad + 2) if at < count]
                right.append(jnp.concatenate(parts, axis=0))
            both = lax.dot_general(
                jnp.concatenate(left, axis=1),
                jnp.concatenate(right, axis=1),
                (((1,), (1,)), ((), ())),
                preferred_element_type=jnp.float32,
            )
            found = found + both[:1, :size]
            if both.shape[1] > size:
                found = found + both[1:2, size:]
        results.append(found)
    lane = lax.broadcasted_iota(jnp.int32, (size, size), 1)
    line = lax.broadcasted_iota(jnp.int32, (size, size), 0)
    for place, row in enumerate(plan.plain):
        total = jnp.zeros((size, size), jnp.float32)
        for number in range(count):
            at = plan.spot(row, number)
            if opening:
                values = block(row, number).astype(jnp.float32)
                wide_ref[place, number] = values
            else:
                values = wide_ref[place, number]
            total = total + values * gather_ref[at : at + 1, :]
        sums = jnp.sum(total, axis=1, keepdims=True)
        results.append(jnp.sum(jnp.where(lane == line, sums, 0.0), axis=0, keepdims=True))
    return jnp.concatenate(results, axis=0)


def opening_kernel(
    plan, received_ref, blocks_ref, want_ref, start_ref, rhs_ref,
    pay_ref, select_ref, wide_ref, smoothed_ref, remainder_ref, search_ref,
    gather_ref, stage_ref, rows_ref, table_ref, spread_ref,
):
    for device in range(plan.devices):
        here = slice(device * plan.rows, (device + 1) * plan.rows)
        values = received_ref[device].astype(jnp.float32)
        rows_ref[here, :] = values[: plan.rows]
        stage_ref[here, :] = values[plan.rows :]
    selection(plan, stage_ref[...].astype(jnp.int32), want_ref[...], table_ref, spread_ref, select_ref)
    remainder = rhs_ref[...] - product(
        plan, blocks_ref, wide_ref, Rounded(rows_ref), select_ref, gather_ref, opening=True
    )
    search = remainder / CENTER
    send(search, pay_ref)
    remainder_ref[...] = remainder
    search_ref[...] = search
    smoothed_ref[...] = start_ref[...] + search


def turn_kernel(
    plan, factors, received_ref, blocks_ref, wide_ref, select_ref, smoothed_in, remainder_in, search_in,
    pay_ref, smoothed_ref, remainder_ref, *rest,
):
    *search_ref, gather_ref = rest
    remainder = remainder_in[...] - product(
        plan, blocks_ref, wide_ref, received_ref, select_ref, gather_ref
    )
    search = factors[0] * search_in[...] + factors[1] * remainder
    send(search, pay_ref)
    remainder_ref[...] = remainder
    smoothed_ref[...] = smoothed_in[...] + search
    if search_ref:
        search_ref[0][...] = search


def closing_kernel(
    plan, received_ref, blocks_ref, wide_ref, select_ref, smoothed_in, remainder_in,
    smoothed_ref, remainder_ref, gather_ref,
):
    smoothed_ref[...] = smoothed_in[...]
    remainder_ref[...] = remainder_in[...] - product(
        plan, blocks_ref, wide_ref, received_ref, select_ref, gather_ref
    )


def local(blocks, pattern, order, start, rhs):
    plan = Plan([lax.axis_size(axis) for axis in ("gx", "gy", "gz")], start.shape)
    state = jax.ShapeDtypeStruct((plan.rows, plan.width), jnp.float32)
    select = jax.ShapeDtypeStruct((plan.lines, plan.sources), jnp.bfloat16)
    gather = [pltpu.VMEM((plan.lines, plan.width), jnp.float32)]
    tables = [
        pltpu.VMEM((plan.sources, plan.width), jnp.float32),
        pltpu.VMEM((plan.sources, plan.width), jnp.float32),
        pltpu.VMEM((plan.targets, LANES), jnp.float32),
        pltpu.VMEM((plan.lines, plan.sources), jnp.float32),
    ]

    def pay(rows):
        return jax.ShapeDtypeStruct((plan.devices, rows, plan.width), jnp.bfloat16)

    def call(kernel, ins, outs, scratch_shapes, cost=None):
        return pl.pallas_call(
            kernel,
            in_specs=ins,
            out_specs=[VMEM] * len(outs),
            out_shape=outs,
            scratch_shapes=scratch_shapes,
            compiler_params=pltpu.CompilerParams(vmem_limit_bytes=GRANT),
            cost_estimate=cost,
        )

    def exchange(sent):
        return lax.all_to_all(sent, AXES, 0, 0, tiled=True)

    def packed(received):
        return received.reshape(plan.sources, plan.width)

    flat_start = start.reshape(state.shape)
    flat_rhs = rhs.reshape(state.shape)
    sent, want = call(
        functools.partial(first_kernel, plan),
        [HBM, HBM, HBM],
        [pay(2 * plan.rows), jax.ShapeDtypeStruct((1, plan.targets), jnp.int32)],
        [
            pltpu.VMEM(state.shape, jnp.float32),
            pltpu.SMEM(order.shape, jnp.int32),
            pltpu.VMEM(pattern.shape, jnp.int32),
            pltpu.SemaphoreType.DMA((3,)),
        ],
        pl.CostEstimate(flops=10**10, bytes_accessed=10**8, transcendentals=0),
    )(far(order), far(pattern), far(flat_start))
    wide = (len(plan.plain), len(plan.entries), plan.width, plan.width)
    wide = jax.ShapeDtypeStruct(wide, jnp.float32)
    sent, table, wide, smoothed, remainder, search = call(
        functools.partial(opening_kernel, plan),
        [VMEM] * 5,
        [pay(plan.rows), select, wide, state, state, state],
        gather + tables,
    )(exchange(sent), blocks, want, flat_start, flat_rhs)
    sigma = CENTER / SPREAD
    rho = 1.0 / sigma
    search = [search]
    for number in range(DEG - 1):
        following = 1.0 / (2.0 * sigma - rho)
        factors = (following * rho, 2.0 * following / SPREAD)
        rho = following
        states = [state] * (3 if number + 2 < DEG else 2)
        sent, smoothed, remainder, *search = call(
            functools.partial(turn_kernel, plan, factors),
            [VMEM] * 7,
            [pay(plan.rows)] + states,
            gather,
        )(packed(exchange(sent)), blocks, wide, table, smoothed, remainder, *search)
    smoothed, remainder = call(
        functools.partial(closing_kernel, plan), [VMEM] * 6, [state, state], gather
    )(packed(exchange(sent)), blocks, wide, table, smoothed, remainder)
    return smoothed.reshape(start.shape), remainder.reshape(start.shape)


def solution(mesh):
    in_specs = (
        P("gx", "gy", "gz", None, None, None),
        P("gx", "gy", None, None),
        P("gx", "gy", None),
        P("gx", "gy", "gz", None),
        P("gx", "gy", "gz", None),
    )
    out_specs = (P("gx", "gy", "gz", None), P("gx", "gy", "gz", None))
    return jax.shard_map(local, mesh=mesh, in_specs=in_specs, out_specs=out_specs, check_vma=False)
```

```python
import functools

import jax
import jax.numpy as jnp
from jax import lax
from jax.experimental import pallas as pl
from jax.experimental.pallas import tpu as pltpu
from jax.sharding import PartitionSpec as P

DEG = 4
CENTER = 1.0
SPREAD = 0.8
LANES = 128
PITCH = 32
GRANT = 16 * 2**20
AXES = ("gz", "gx", "gy")
VMEM = pl.BlockSpec(memory_space=pltpu.VMEM)
HBM = pl.BlockSpec(memory_space=pltpu.HBM)


def far(array):
    return pltpu.with_memory_space_constraint(array, pltpu.HBM)


class Plan:
    def __init__(self, axis_sizes, local_shape):
        self.gx, self.gy, self.gz = axis_sizes
        self.nx, self.ny, self.nz, self.width = local_shape
        self.devices = self.gx * self.gy * self.gz
        self.rows = self.nx * self.ny * self.nz
        self.sources = self.devices * self.rows
        self.few = self.ny == 1 and self.gy <= 2
        self.spans = min(3, self.gy) if self.few else 3
        self.entries = [(i, j, k) for i in range(3) for j in range(self.spans) for k in range(3)]
        self.targets = -(-self.rows * PITCH // LANES) * LANES
        self.tiled = list(range(self.rows // 4))
        self.plain = list(range(self.rows // 4, self.rows))
        self.quads = -(-len(self.entries) // 4)
        self.depth = self.gz * self.nz
        self.high = -(-self.depth // 8) * 8
        self.across = self.spans if self.few else self.ny + 2
        self.columns = (self.nx + 2) * self.across
        self.picks = [
            (row, i, j) for row in range(self.rows) for i in range(3) for j in range(self.spans)
        ]

    def first_span(self):
        return 1 - lax.axis_index("gy") if self.few else 0

    def place(self, row):
        return row // (self.ny * self.nz), row // self.nz % self.ny, row % self.nz

    def spot(self, row, number):
        i, j, k = self.entries[number]
        return 8 * ((row * 3 + i) * self.spans + j) + k

    def column(self, row, i, j):
        x, y, _ = self.place(row)
        return (x + i) * self.across + (j if self.few else y + j)

    def beside(self, number, count, axis, devices):
        me = lax.axis_index(axis)
        if number == 0:
            return jnp.maximum(me - 1, 0), count - 1, me > 0
        if number == count + 1:
            return jnp.minimum(me + 1, devices - 1), 0, me < devices - 1
        return me, number - 1, None


def send(tile, pay_ref):
    pay_ref[...] = jnp.broadcast_to(tile.astype(jnp.bfloat16)[None], pay_ref.shape)


def first_kernel(
    plan, order_hbm, pattern_hbm, start_hbm,
    pay_ref, plane_ref, keep_ref, start_ref, order_ref, pattern_ref, sems,
):
    copies = (
        pltpu.make_async_copy(order_hbm, order_ref, sems.at[0]),
        pltpu.make_async_copy(pattern_hbm, pattern_ref, sems.at[1]),
        pltpu.make_async_copy(start_hbm, start_ref, sems.at[2]),
    )
    for copy in copies:
        copy.start()
    for copy in copies:
        copy.wait()
    first = lax.axis_index("gz") * plan.nz
    line = lax.broadcasted_iota(jnp.int32, (plan.rows, plan.width), 0)
    planes = jnp.zeros_like(line)
    for row in range(plan.rows):
        x, y, s = plan.place(row)
        planes = jnp.where(line == row, order_ref[x, y, first + s], planes)
    planes = planes.astype(jnp.float32)
    send(jnp.concatenate([start_ref[...], planes], axis=0), pay_ref)
    plane_ref[...] = planes
    keep_ref[...] = kept(plan, pattern_ref)


def kept(plan, pattern_ref):
    first = lax.axis_index("gz") * plan.nz
    span = plan.first_span()
    lane = lax.broadcasted_iota(jnp.int32, (1, plan.targets), 1)
    flat = jnp.zeros_like(lane)
    for number in range(plan.rows):
        x, y, s = plan.place(number)
        flags = pattern_ref[x, y, pl.ds(first + s, 1), :]
        gap = jnp.zeros((1, plan.targets - flags.shape[1]), jnp.int32)
        flags = jnp.concatenate([flags, gap], axis=1)
        turn = lax.rem(plan.targets + PITCH * number - 3 * span, plan.targets)
        flat = flat + pltpu.roll(flags, turn, 1)
    centre = (lane & (PITCH - 1)) + 3 * span == 13
    return jnp.where((flat > 0) | centre, 1.0, 0.0)


def gathered_columns(plan, received_ref, base):
    loaded = {}
    columns = []
    for i in range(plan.nx + 2):
        device_x, x, _ = plan.beside(i, plan.nx, "gx", plan.gx)
        side = (i > 0) + (i > plan.nx)
        for j in range(plan.across):
            if plan.few:
                device_y, y, slice_y = j, 0, j
            else:
                device_y, y, _ = plan.beside(j, plan.ny, "gy", plan.gy)
                slice_y = (j > 0) + (j > plan.ny)
            parts = []
            for z in range(plan.gz):
                name = (side, slice_y, z)
                if name not in loaded:
                    device = (z * plan.gx + device_x) * plan.gy + device_y
                    loaded[name] = received_ref[device].astype(jnp.float32)
                low = base + (x * plan.ny + y) * plan.nz
                parts.append(loaded[name][low : low + plan.nz])
            if plan.high > plan.depth:
                parts.append(jnp.zeros((plan.high - plan.depth, plan.width), jnp.float32))
            columns.append(jnp.concatenate(parts, axis=0))
    return columns


def pick(column, index):
    high = column.shape[0]
    numbers = lax.GatherDimensionNumbers(
        offset_dims=(),
        collapsed_slice_dims=(0,),
        start_index_map=(0,),
        operand_batching_dims=(1,),
        start_indices_batching_dims=(1,),
    )
    found = None
    for group in range(high // 8):
        part = lax.gather(
            column[8 * group : 8 * group + 8],
            (index if high == 8 else index & 7)[..., None],
            numbers,
            (1, 1),
            mode=lax.GatherScatterMode.PROMISE_IN_BOUNDS,
        )
        found = part if found is None else jnp.where(index >> 3 == group, part, found)
    return found


def tables(plan, columns, plane_ref, keep_ref, slots_ref, flags_ref, index_ref, mask_ref):
    for first in range(0, plan.targets, LANES):
        part = jnp.broadcast_to(keep_ref[:, first : first + LANES], (LANES, LANES))
        flags_ref[first : first + LANES, :] = part.T
    line = lax.broadcasted_iota(jnp.int32, (plan.high, LANES), 0).astype(jnp.float32)
    inverses = []
    for number, column in enumerate(columns):
        slots_ref[number] = column
        inverse = jnp.zeros((plan.high, LANES), jnp.int32)
        for slot in range(plan.depth):
            inverse = jnp.where(slots_ref[number, slot : slot + 1, :] == line, slot, inverse)
        inverses.append(inverse)
    step = lax.broadcasted_iota(jnp.int32, (8, LANES), 0).astype(jnp.float32) - 1.0
    for place, (row, i, j) in enumerate(plan.picks):
        x, y, _ = plan.place(row)
        want = plane_ref[row : row + 1, :] + step
        inside = (want >= 0.0) & (want < plan.depth) & (step < 2.0)
        want = jnp.clip(want, 0.0, plan.depth - 1.0).astype(jnp.int32)
        at = row * PITCH + 9 * i + 3 * j
        mask = jnp.where(inside, flags_ref[at : at + 8, :], 0.0)
        _, _, on_grid = plan.beside(x + i, plan.nx, "gx", plan.gx)
        if on_grid is not None:
            mask = jnp.where(on_grid, mask, 0.0)
        if not plan.few:
            _, _, on_grid = plan.beside(y + j, plan.ny, "gy", plan.gy)
            if on_grid is not None:
                mask = jnp.where(on_grid, mask, 0.0)
        at = 8 * place
        index_ref[at : at + 8, :] = pick(inverses[plan.column(row, i, j)], want)
        mask_ref[at : at + 8, :] = mask


def block_of(plan, blocks_ref, row, number):
    x, y, s = plan.place(row)
    i, j, k = plan.entries[number]
    return blocks_ref[x, y, s, 9 * i + 3 * (j + plan.first_span()) + k]


def product(plan, blocks_ref, wide_ref, received_ref, index_ref, mask_ref, gather_ref, opening=False):
    columns = gathered_columns(plan, received_ref, 0)
    for place, (row, i, j) in enumerate(plan.picks):
        here = slice(8 * place, 8 * place + 8)
        values = pick(columns[plan.column(row, i, j)], index_ref[here, :])
        gather_ref[here, :] = values * mask_ref[here, :]
    size = plan.width
    count = len(plan.entries)
    block = functools.partial(block_of, plan, blocks_ref)

    def pair(row, number):
        blank = jnp.zeros((size, size), jnp.bfloat16)
        sides = [block(row, at) if at < count else blank for at in (number, number + 1)]
        return jnp.concatenate(sides, axis=1)

    def vectors(row, number):
        if number >= count:
            return jnp.zeros((1, size), jnp.float32)
        at = plan.spot(row, number)
        return gather_ref[at : at + 1, :]

    results = []
    for row in plan.tiled:
        found = jnp.zeros((1, size), jnp.float32)
        whole = [quad for quad in range(plan.quads) if 4 * quad + 2 < count]
        cut = len(whole) // 2
        for group in (whole[:cut], whole[cut:], [plan.quads - 1] if plan.quads > len(whole) else []):
            if not group:
                continue
            left, right = [], []
            for quad in group:
                for side in (0, 1):
                    lines = [vectors(row, 4 * quad + side), vectors(row, 4 * quad + 2 + side)]
                    left.append(jnp.concatenate(lines, axis=0).astype(jnp.bfloat16))
                parts = [pair(row, at) for at in (4 * quad, 4 * quad + 2) if at < count]
                right.append(jnp.concatenate(parts, axis=0))
            both = lax.dot_general(
                jnp.concatenate(left, axis=1),
                jnp.concatenate(right, axis=1),
                (((1,), (1,)), ((), ())),
                preferred_element_type=jnp.float32,
            )
            found = found + both[:1, :size]
            if both.shape[1] > size:
                found = found + both[1:2, size:]
        results.append(found)
    lane = lax.broadcasted_iota(jnp.int32, (size, size), 1)
    line = lax.broadcasted_iota(jnp.int32, (size, size), 0)
    for place, row in enumerate(plan.plain):
        total = jnp.zeros((size, size), jnp.float32)
        for number in range(count):
            if opening:
                values = block(row, number).astype(jnp.float32)
                wide_ref[place, number] = values
            else:
                values = wide_ref[place, number]
            total = total + values * vectors(row, number)
        sums = jnp.sum(total, axis=1, keepdims=True)
        results.append(jnp.sum(jnp.where(lane == line, sums, 0.0), axis=0, keepdims=True))
    return jnp.concatenate(results, axis=0)


def opening_kernel(
    plan, received_ref, blocks_ref, plane_ref, keep_ref, start_ref, rhs_ref,
    pay_ref, index_ref, mask_ref, wide_ref, smoothed_ref, remainder_ref, search_ref,
    gather_ref, slots_ref, flags_ref,
):
    columns = gathered_columns(plan, received_ref, plan.rows)
    tables(plan, columns, plane_ref, keep_ref, slots_ref, flags_ref, index_ref, mask_ref)
    remainder = rhs_ref[...] - product(
        plan, blocks_ref, wide_ref, received_ref, index_ref, mask_ref, gather_ref, True
    )
    search = remainder / CENTER
    send(search, pay_ref)
    remainder_ref[...] = remainder
    search_ref[...] = search
    smoothed_ref[...] = start_ref[...] + search


def turn_kernel(
    plan, factors, received_ref, blocks_ref, wide_ref, index_ref, mask_ref,
    smoothed_in, remainder_in, search_in,
    pay_ref, smoothed_ref, remainder_ref, *rest,
):
    *search_ref, gather_ref = rest
    remainder = remainder_in[...] - product(
        plan, blocks_ref, wide_ref, received_ref, index_ref, mask_ref, gather_ref
    )
    search = factors[0] * search_in[...] + factors[1] * remainder
    send(search, pay_ref)
    remainder_ref[...] = remainder
    smoothed_ref[...] = smoothed_in[...] + search
    if search_ref:
        search_ref[0][...] = search


def closing_kernel(
    plan, received_ref, blocks_ref, wide_ref, index_ref, mask_ref, smoothed_in, remainder_in,
    smoothed_ref, remainder_ref, gather_ref,
):
    smoothed_ref[...] = smoothed_in[...]
    remainder_ref[...] = remainder_in[...] - product(
        plan, blocks_ref, wide_ref, received_ref, index_ref, mask_ref, gather_ref
    )


def local(blocks, pattern, order, start, rhs):
    plan = Plan([lax.axis_size(axis) for axis in ("gx", "gy", "gz")], start.shape)
    width = plan.width

    def like(kind, *shape):
        return jax.ShapeDtypeStruct(shape, kind)

    def pay(rows):
        return like(jnp.bfloat16, plan.devices, rows, width)

    state = like(jnp.float32, plan.rows, width)
    scratch = [pltpu.VMEM((8 * len(plan.picks), width), jnp.float32)]

    def call(kernel, ins, outs, scratch_shapes, cost=None):
        return pl.pallas_call(
            kernel,
            in_specs=ins,
            out_specs=[VMEM] * len(outs),
            out_shape=outs,
            scratch_shapes=scratch_shapes,
            compiler_params=pltpu.CompilerParams(vmem_limit_bytes=GRANT),
            cost_estimate=cost,
        )

    def exchange(sent):
        return lax.all_to_all(sent, AXES, 0, 0, tiled=True)

    flat_start = start.reshape(state.shape)
    flat_rhs = rhs.reshape(state.shape)
    sent, plane, keep = call(
        functools.partial(first_kernel, plan),
        [HBM, HBM, HBM],
        [pay(2 * plan.rows), state, like(jnp.float32, 1, plan.targets)],
        [
            pltpu.VMEM(state.shape, jnp.float32),
            pltpu.SMEM(order.shape, jnp.int32),
            pltpu.VMEM(pattern.shape, jnp.int32),
            pltpu.SemaphoreType.DMA((3,)),
        ],
        pl.CostEstimate(flops=10**10, bytes_accessed=10**8, transcendentals=0),
    )(far(order), far(pattern), far(flat_start))
    sent, index, mask, wide, smoothed, remainder, *search = call(
        functools.partial(opening_kernel, plan),
        [VMEM] * 6,
        [
            pay(plan.rows),
            like(jnp.int32, 8 * len(plan.picks), LANES),
            like(jnp.float32, 8 * len(plan.picks), LANES),
            like(jnp.float32, len(plan.plain), len(plan.entries), width, width),
            state,
            state,
            state,
        ],
        scratch
        + [
            pltpu.VMEM((plan.columns, plan.high, LANES), jnp.float32),
            pltpu.VMEM((plan.targets, LANES), jnp.float32),
        ],
    )(exchange(sent), blocks, plane, keep, flat_start, flat_rhs)
    sigma = CENTER / SPREAD
    rho = 1.0 / sigma
    for number in range(DEG - 1):
        following = 1.0 / (2.0 * sigma - rho)
        factors = (following * rho, 2.0 * following / SPREAD)
        rho = following
        states = [state] * (3 if number + 2 < DEG else 2)
        sent, smoothed, remainder, *search = call(
            functools.partial(turn_kernel, plan, factors),
            [VMEM] * 8,
            [pay(plan.rows)] + states,
            scratch,
        )(exchange(sent), blocks, wide, index, mask, smoothed, remainder, *search)
    smoothed, remainder = call(
        functools.partial(closing_kernel, plan), [VMEM] * 7, [state, state], scratch
    )(exchange(sent), blocks, wide, index, mask, smoothed, remainder)
    return smoothed.reshape(start.shape), remainder.reshape(start.shape)


def solution(mesh):
    in_specs = (
        P("gx", "gy", "gz", None, None, None),
        P("gx", "gy", None, None),
        P("gx", "gy", None),
        P("gx", "gy", "gz", None),
        P("gx", "gy", "gz", None),
    )
    out_specs = (P("gx", "gy", "gz", None), P("gx", "gy", "gz", None))
    return jax.shard_map(local, mesh=mesh, in_specs=in_specs, out_specs=out_specs, check_vma=False)
```

```python
import functools

import jax
import jax.numpy as jnp
from jax import lax
from jax.experimental import pallas as pl
from jax.experimental.pallas import tpu as pltpu
from jax.sharding import PartitionSpec as P

DEG = 4
CENTER = 1.0
SPREAD = 0.8
LANES = 128
PITCH = 32
GRANT = 16 * 2**20
AXES = ("gz", "gx", "gy")
VMEM = pl.BlockSpec(memory_space=pltpu.VMEM)
HBM = pl.BlockSpec(memory_space=pltpu.HBM)


def far(array):
    return pltpu.with_memory_space_constraint(array, pltpu.HBM)


class Plan:
    def __init__(self, axis_sizes, local_shape):
        self.gx, self.gy, self.gz = axis_sizes
        self.nx, self.ny, self.nz, self.width = local_shape
        self.devices = self.gx * self.gy * self.gz
        self.rows = self.nx * self.ny * self.nz
        self.sources = self.devices * self.rows
        self.few = self.ny == 1 and self.gy <= 2
        self.spans = min(3, self.gy) if self.few else 3
        self.entries = [(i, j, k) for i in range(3) for j in range(self.spans) for k in range(3)]
        self.targets = -(-self.rows * PITCH // LANES) * LANES
        self.tiled = list(range(self.rows // 4))
        self.plain = list(range(self.rows // 4, self.rows))
        self.quads = -(-len(self.entries) // 4)
        self.depth = self.gz * self.nz
        self.high = -(-self.depth // 8) * 8
        self.across = self.spans if self.few else self.ny + 2
        self.columns = (self.nx + 2) * self.across
        self.picks = [
            (row, i, j) for row in range(self.rows) for i in range(3) for j in range(self.spans)
        ]

    def first_span(self):
        return 1 - lax.axis_index("gy") if self.few else 0

    def place(self, row):
        return row // (self.ny * self.nz), row // self.nz % self.ny, row % self.nz

    def spot(self, row, number):
        i, j, k = self.entries[number]
        return 8 * ((row * 3 + i) * self.spans + j) + k

    def column(self, row, i, j):
        x, y, _ = self.place(row)
        return (x + i) * self.across + (j if self.few else y + j)

    def beside(self, number, count, axis, devices):
        me = lax.axis_index(axis)
        if number == 0:
            return jnp.maximum(me - 1, 0), count - 1, me > 0
        if number == count + 1:
            return jnp.minimum(me + 1, devices - 1), 0, me < devices - 1
        return me, number - 1, None


def send(tile, pay_ref):
    pay_ref[...] = jnp.broadcast_to(tile.astype(jnp.bfloat16)[None], pay_ref.shape)


def first_kernel(
    plan, order_hbm, pattern_hbm, start_hbm,
    pay_ref, plane_ref, keep_ref, start_ref, order_ref, pattern_ref, sems,
):
    copies = (
        pltpu.make_async_copy(order_hbm, order_ref, sems.at[0]),
        pltpu.make_async_copy(pattern_hbm, pattern_ref, sems.at[1]),
        pltpu.make_async_copy(start_hbm, start_ref, sems.at[2]),
    )
    for copy in copies:
        copy.start()
    for copy in copies:
        copy.wait()
    first = lax.axis_index("gz") * plan.nz
    line = lax.broadcasted_iota(jnp.int32, (plan.rows, plan.width), 0)
    planes = jnp.zeros_like(line)
    for row in range(plan.rows):
        x, y, s = plan.place(row)
        planes = jnp.where(line == row, order_ref[x, y, first + s], planes)
    planes = planes.astype(jnp.float32)
    send(jnp.concatenate([start_ref[...], planes], axis=0), pay_ref)
    plane_ref[...] = planes
    keep_ref[...] = kept(plan, pattern_ref)


def kept(plan, pattern_ref):
    first = lax.axis_index("gz") * plan.nz
    span = plan.first_span()
    lane = lax.broadcasted_iota(jnp.int32, (1, plan.targets), 1)
    flat = jnp.zeros_like(lane)
    for number in range(plan.rows):
        x, y, s = plan.place(number)
        flags = pattern_ref[x, y, pl.ds(first + s, 1), :]
        gap = jnp.zeros((1, plan.targets - flags.shape[1]), jnp.int32)
        flags = jnp.concatenate([flags, gap], axis=1)
        turn = lax.rem(plan.targets + PITCH * number - 3 * span, plan.targets)
        flat = flat + pltpu.roll(flags, turn, 1)
    centre = (lane & (PITCH - 1)) + 3 * span == 13
    return jnp.where((flat > 0) | centre, 1.0, 0.0)


def gathered_columns(plan, received_ref, base):
    loaded = {}
    columns = []
    for i in range(plan.nx + 2):
        device_x, x, _ = plan.beside(i, plan.nx, "gx", plan.gx)
        side = (i > 0) + (i > plan.nx)
        for j in range(plan.across):
            if plan.few:
                device_y, y, slice_y = j, 0, j
            else:
                device_y, y, _ = plan.beside(j, plan.ny, "gy", plan.gy)
                slice_y = (j > 0) + (j > plan.ny)
            parts = []
            for z in range(plan.gz):
                name = (side, slice_y, z)
                if name not in loaded:
                    device = (z * plan.gx + device_x) * plan.gy + device_y
                    loaded[name] = received_ref[device].astype(jnp.float32)
                low = base + (x * plan.ny + y) * plan.nz
                parts.append(loaded[name][low : low + plan.nz])
            if plan.high > plan.depth:
                parts.append(jnp.zeros((plan.high - plan.depth, plan.width), jnp.float32))
            columns.append(jnp.concatenate(parts, axis=0))
    return columns


def pick(column, index):
    high = column.shape[0]
    numbers = lax.GatherDimensionNumbers(
        offset_dims=(),
        collapsed_slice_dims=(0,),
        start_index_map=(0,),
        operand_batching_dims=(1,),
        start_indices_batching_dims=(1,),
    )
    found = None
    for group in range(high // 8):
        part = lax.gather(
            column[8 * group : 8 * group + 8],
            (index if high == 8 else index & 7)[..., None],
            numbers,
            (1, 1),
            mode=lax.GatherScatterMode.PROMISE_IN_BOUNDS,
        )
        found = part if found is None else jnp.where(index >> 3 == group, part, found)
    return found


def tables(plan, columns, plane_ref, keep_ref, slots_ref, flags_ref, index_ref, mask_ref):
    for first in range(0, plan.targets, LANES):
        part = jnp.broadcast_to(keep_ref[:, first : first + LANES], (LANES, LANES))
        flags_ref[first : first + LANES, :] = part.T
    line = lax.broadcasted_iota(jnp.int32, (plan.high, LANES), 0).astype(jnp.float32)
    inverses = []
    for number, column in enumerate(columns):
        slots_ref[number] = column
        inverse = jnp.zeros((plan.high, LANES), jnp.int32)
        for slot in range(plan.depth):
            inverse = jnp.where(slots_ref[number, slot : slot + 1, :] == line, slot, inverse)
        inverses.append(inverse)
    step = lax.broadcasted_iota(jnp.int32, (8, LANES), 0).astype(jnp.float32) - 1.0
    for place, (row, i, j) in enumerate(plan.picks):
        x, y, _ = plan.place(row)
        want = plane_ref[row : row + 1, :] + step
        inside = (want >= 0.0) & (want < plan.depth) & (step < 2.0)
        want = jnp.clip(want, 0.0, plan.depth - 1.0).astype(jnp.int32)
        at = row * PITCH + 9 * i + 3 * j
        mask = jnp.where(inside, flags_ref[at : at + 8, :], 0.0)
        _, _, on_grid = plan.beside(x + i, plan.nx, "gx", plan.gx)
        if on_grid is not None:
            mask = jnp.where(on_grid, mask, 0.0)
        if not plan.few:
            _, _, on_grid = plan.beside(y + j, plan.ny, "gy", plan.gy)
            if on_grid is not None:
                mask = jnp.where(on_grid, mask, 0.0)
        at = 8 * place
        index_ref[at : at + 8, :] = pick(inverses[plan.column(row, i, j)], want)
        mask_ref[at : at + 8, :] = mask


def block_of(plan, blocks_ref, row, number):
    x, y, s = plan.place(row)
    i, j, k = plan.entries[number]
    return blocks_ref[x, y, s, 9 * i + 3 * (j + plan.first_span()) + k]


def tile_of(plan, block, row, group, tile_ref):
    size = plan.width
    for quad in group:
        for part in range(4):
            number = 4 * quad + part
            line = size * (2 * quad + part % 2)
            lane = size * (part // 2)
            if number < len(plan.entries):
                values = block(row, number).astype(jnp.float32).T.astype(jnp.bfloat16)
            else:
                values = jnp.zeros((size, size), jnp.bfloat16)
            tile_ref[row, line : line + size, lane : lane + size] = values


def product(plan, blocks_ref, tile_ref, wide_ref, received_ref, index_ref, mask_ref, gather_ref, opening=False):
    columns = gathered_columns(plan, received_ref, 0)
    for place, (row, i, j) in enumerate(plan.picks):
        here = slice(8 * place, 8 * place + 8)
        values = pick(columns[plan.column(row, i, j)], index_ref[here, :])
        gather_ref[here, :] = values * mask_ref[here, :]
    size = plan.width
    count = len(plan.entries)
    block = functools.partial(block_of, plan, blocks_ref)

    def pair(row, number):
        blank = jnp.zeros((size, size), jnp.bfloat16)
        sides = [block(row, at) if at < count else blank for at in (number, number + 1)]
        return jnp.concatenate(sides, axis=1)

    def vectors(row, number):
        if number >= count:
            return jnp.zeros((1, size), jnp.float32)
        at = plan.spot(row, number)
        return gather_ref[at : at + 1, :]

    results = []
    for row in plan.tiled:
        found = jnp.zeros((1, size), jnp.float32)
        whole = [quad for quad in range(plan.quads) if 4 * quad + 2 < count]
        cut = len(whole) // 2
        for group in (whole[:cut], whole[cut:], [plan.quads - 1] if plan.quads > len(whole) else []):
            if not group:
                continue
            if opening:
                tile_of(plan, block, row, group, tile_ref)
            left, right = [], []
            for quad in group:
                for side in (0, 1):
                    lines = [vectors(row, 4 * quad + side), vectors(row, 4 * quad + 2 + side)]
                    left.append(jnp.concatenate(lines, axis=0).astype(jnp.bfloat16))
                if opening:
                    parts = [pair(row, at) for at in (4 * quad, 4 * quad + 2) if at < count]
                    right.append(jnp.concatenate(parts, axis=0))
            left = jnp.concatenate(left, axis=1)
            if opening:
                both = lax.dot_general(
                    left,
                    jnp.concatenate(right, axis=1),
                    (((1,), (1,)), ((), ())),
                    preferred_element_type=jnp.float32,
                )
            else:
                here = slice(2 * size * group[0], 2 * size * (group[-1] + 1))
                both = jnp.dot(left, tile_ref[row, here, :], preferred_element_type=jnp.float32)
            found = found + both[:1, :size]
            if both.shape[1] > size:
                found = found + both[1:2, size:]
        results.append(found)
    for place, row in enumerate(plan.plain):
        total = jnp.zeros((size, size), jnp.float32)
        for number in range(count):
            if opening:
                values = block(row, number).astype(jnp.float32)
                wide_ref[place, number] = values
            else:
                values = wide_ref[place, number]
            total = total + values * vectors(row, number)
        high = total.astype(jnp.bfloat16)
        low = (total - high.astype(jnp.float32)).astype(jnp.bfloat16)
        sums = lax.dot_general(
            jnp.ones((8, 2 * size), jnp.bfloat16),
            jnp.concatenate([high, low], axis=1),
            (((1,), (1,)), ((), ())),
            preferred_element_type=jnp.float32,
        )
        results.append(sums[:1])
    return jnp.concatenate(results, axis=0)


def opening_kernel(
    plan, received_ref, blocks_ref, plane_ref, keep_ref, start_ref, rhs_ref,
    pay_ref, index_ref, mask_ref, tile_ref, wide_ref, smoothed_ref, remainder_ref, search_ref,
    gather_ref, slots_ref, flags_ref,
):
    columns = gathered_columns(plan, received_ref, plan.rows)
    tables(plan, columns, plane_ref, keep_ref, slots_ref, flags_ref, index_ref, mask_ref)
    remainder = rhs_ref[...] - product(
        plan, blocks_ref, tile_ref, wide_ref, received_ref, index_ref, mask_ref, gather_ref, True
    )
    search = remainder / CENTER
    send(search, pay_ref)
    remainder_ref[...] = remainder
    search_ref[...] = search
    smoothed_ref[...] = start_ref[...] + search


def turn_kernel(
    plan, factors, received_ref, tile_ref, wide_ref, index_ref, mask_ref,
    smoothed_in, remainder_in, search_in,
    pay_ref, smoothed_ref, remainder_ref, *rest,
):
    *search_ref, gather_ref = rest
    remainder = remainder_in[...] - product(
        plan, None, tile_ref, wide_ref, received_ref, index_ref, mask_ref, gather_ref
    )
    search = factors[0] * search_in[...] + factors[1] * remainder
    send(search, pay_ref)
    remainder_ref[...] = remainder
    smoothed_ref[...] = smoothed_in[...] + search
    if search_ref:
        search_ref[0][...] = search


def closing_kernel(
    plan, received_ref, tile_ref, wide_ref, index_ref, mask_ref, smoothed_in, remainder_in,
    smoothed_ref, remainder_ref, gather_ref,
):
    smoothed_ref[...] = smoothed_in[...]
    remainder_ref[...] = remainder_in[...] - product(
        plan, None, tile_ref, wide_ref, received_ref, index_ref, mask_ref, gather_ref
    )


def local(blocks, pattern, order, start, rhs):
    plan = Plan([lax.axis_size(axis) for axis in ("gx", "gy", "gz")], start.shape)
    width = plan.width

    def like(kind, *shape):
        return jax.ShapeDtypeStruct(shape, kind)

    def pay(rows):
        return like(jnp.bfloat16, plan.devices, rows, width)

    state = like(jnp.float32, plan.rows, width)
    scratch = [pltpu.VMEM((8 * len(plan.picks), width), jnp.float32)]

    def call(kernel, ins, outs, scratch_shapes, cost=None):
        return pl.pallas_call(
            kernel,
            in_specs=ins,
            out_specs=[VMEM] * len(outs),
            out_shape=outs,
            scratch_shapes=scratch_shapes,
            compiler_params=pltpu.CompilerParams(vmem_limit_bytes=GRANT),
            cost_estimate=cost,
        )

    def exchange(sent):
        return lax.all_to_all(sent, AXES, 0, 0, tiled=True)

    flat_start = start.reshape(state.shape)
    flat_rhs = rhs.reshape(state.shape)
    sent, plane, keep = call(
        functools.partial(first_kernel, plan),
        [HBM, HBM, HBM],
        [pay(2 * plan.rows), state, like(jnp.float32, 1, plan.targets)],
        [
            pltpu.VMEM(state.shape, jnp.float32),
            pltpu.SMEM(order.shape, jnp.int32),
            pltpu.VMEM(pattern.shape, jnp.int32),
            pltpu.SemaphoreType.DMA((3,)),
        ],
        pl.CostEstimate(flops=10**10, bytes_accessed=10**8, transcendentals=0),
    )(far(order), far(pattern), far(flat_start))
    sent, index, mask, tile, wide, smoothed, remainder, *search = call(
        functools.partial(opening_kernel, plan),
        [VMEM] * 6,
        [
            pay(plan.rows),
            like(jnp.int32, 8 * len(plan.picks), LANES),
            like(jnp.float32, 8 * len(plan.picks), LANES),
            like(jnp.bfloat16, len(plan.tiled), 2 * width * plan.quads, 2 * width),
            like(jnp.float32, len(plan.plain), len(plan.entries), width, width),
            state,
            state,
            state,
        ],
        scratch
        + [
            pltpu.VMEM((plan.columns, plan.high, LANES), jnp.float32),
            pltpu.VMEM((plan.targets, LANES), jnp.float32),
        ],
    )(exchange(sent), blocks, plane, keep, flat_start, flat_rhs)
    sigma = CENTER / SPREAD
    rho = 1.0 / sigma
    for number in range(DEG - 1):
        following = 1.0 / (2.0 * sigma - rho)
        factors = (following * rho, 2.0 * following / SPREAD)
        rho = following
        states = [state] * (3 if number + 2 < DEG else 2)
        sent, smoothed, remainder, *search = call(
            functools.partial(turn_kernel, plan, factors),
            [VMEM] * 8,
            [pay(plan.rows)] + states,
            scratch,
        )(exchange(sent), tile, wide, index, mask, smoothed, remainder, *search)
    smoothed, remainder = call(
        functools.partial(closing_kernel, plan), [VMEM] * 7, [state, state], scratch
    )(exchange(sent), tile, wide, index, mask, smoothed, remainder)
    return smoothed.reshape(start.shape), remainder.reshape(start.shape)


def solution(mesh):
    in_specs = (
        P("gx", "gy", "gz", None, None, None),
        P("gx", "gy", None, None),
        P("gx", "gy", None),
        P("gx", "gy", "gz", None),
        P("gx", "gy", "gz", None),
    )
    out_specs = (P("gx", "gy", "gz", None), P("gx", "gy", "gz", None))
    return jax.shard_map(local, mesh=mesh, in_specs=in_specs, out_specs=out_specs, check_vma=False)
```

```python
import functools

import jax
import jax.numpy as jnp
from jax import lax
from jax.experimental import pallas as pl
from jax.experimental.pallas import tpu as pltpu
from jax.sharding import PartitionSpec as P

DEG = 4
CENTER = 1.0
SPREAD = 0.8
LANES = 128
PITCH = 32
GRANT = 16 * 2**20
AXES = ("gz", "gx", "gy")
VMEM = pl.BlockSpec(memory_space=pltpu.VMEM)
HBM = pl.BlockSpec(memory_space=pltpu.HBM)


def far(array):
    return pltpu.with_memory_space_constraint(array, pltpu.HBM)


class Plan:
    def __init__(self, axis_sizes, local_shape):
        self.gx, self.gy, self.gz = axis_sizes
        self.nx, self.ny, self.nz, self.width = local_shape
        self.devices = self.gx * self.gy * self.gz
        self.rows = self.nx * self.ny * self.nz
        self.sources = self.devices * self.rows
        self.few = self.ny == 1 and self.gy <= 2
        self.spans = min(3, self.gy) if self.few else 3
        self.entries = [(i, j, k) for i in range(3) for j in range(self.spans) for k in range(3)]
        self.targets = -(-self.rows * PITCH // LANES) * LANES
        self.tiled = list(range(self.rows // 4))
        self.plain = list(range(self.rows // 4, self.rows))
        self.quads = -(-len(self.entries) // 4)
        self.depth = self.gz * self.nz
        self.high = -(-self.depth // 8) * 8
        self.across = self.spans if self.few else self.ny + 2
        self.columns = (self.nx + 2) * self.across
        self.picks = [
            (row, i, j) for row in range(self.rows) for i in range(3) for j in range(self.spans)
        ]

    def first_span(self):
        return 1 - lax.axis_index("gy") if self.few else 0

    def place(self, row):
        return row // (self.ny * self.nz), row // self.nz % self.ny, row % self.nz

    def spot(self, row, number):
        i, j, k = self.entries[number]
        return 8 * ((row * 3 + i) * self.spans + j) + k

    def column(self, row, i, j):
        x, y, _ = self.place(row)
        return (x + i) * self.across + (j if self.few else y + j)

    def beside(self, number, count, axis, devices):
        me = lax.axis_index(axis)
        if number == 0:
            return jnp.maximum(me - 1, 0), count - 1, me > 0
        if number == count + 1:
            return jnp.minimum(me + 1, devices - 1), 0, me < devices - 1
        return me, number - 1, None


def send(tile, pay_ref):
    pay_ref[...] = jnp.broadcast_to(tile.astype(jnp.bfloat16)[None], pay_ref.shape)


def first_kernel(
    plan, order_hbm, pattern_hbm, start_hbm,
    pay_ref, plane_ref, keep_ref, start_ref, order_ref, pattern_ref, sems,
):
    copies = (
        pltpu.make_async_copy(order_hbm, order_ref, sems.at[0]),
        pltpu.make_async_copy(pattern_hbm, pattern_ref, sems.at[1]),
        pltpu.make_async_copy(start_hbm, start_ref, sems.at[2]),
    )
    for copy in copies:
        copy.start()
    for copy in copies:
        copy.wait()
    first = lax.axis_index("gz") * plan.nz
    line = lax.broadcasted_iota(jnp.int32, (plan.rows, plan.width), 0)
    planes = jnp.zeros_like(line)
    for row in range(plan.rows):
        x, y, s = plan.place(row)
        planes = jnp.where(line == row, order_ref[x, y, first + s], planes)
    planes = planes.astype(jnp.float32)
    send(jnp.concatenate([start_ref[...], planes], axis=0), pay_ref)
    plane_ref[...] = planes
    keep_ref[...] = kept(plan, pattern_ref)


def kept(plan, pattern_ref):
    first = lax.axis_index("gz") * plan.nz
    span = plan.first_span()
    lane = lax.broadcasted_iota(jnp.int32, (1, plan.targets), 1)
    flat = jnp.zeros_like(lane)
    for number in range(plan.rows):
        x, y, s = plan.place(number)
        flags = pattern_ref[x, y, pl.ds(first + s, 1), :]
        gap = jnp.zeros((1, plan.targets - flags.shape[1]), jnp.int32)
        flags = jnp.concatenate([flags, gap], axis=1)
        turn = lax.rem(plan.targets + PITCH * number - 3 * span, plan.targets)
        flat = flat + pltpu.roll(flags, turn, 1)
    centre = (lane & (PITCH - 1)) + 3 * span == 13
    return jnp.where((flat > 0) | centre, 1.0, 0.0)


def gathered_columns(plan, received_ref, base):
    loaded = {}
    columns = []
    for i in range(plan.nx + 2):
        device_x, x, _ = plan.beside(i, plan.nx, "gx", plan.gx)
        side = (i > 0) + (i > plan.nx)
        for j in range(plan.across):
            if plan.few:
                device_y, y, slice_y = j, 0, j
            else:
                device_y, y, _ = plan.beside(j, plan.ny, "gy", plan.gy)
                slice_y = (j > 0) + (j > plan.ny)
            parts = []
            for z in range(plan.gz):
                name = (side, slice_y, z)
                if name not in loaded:
                    device = (z * plan.gx + device_x) * plan.gy + device_y
                    loaded[name] = received_ref[device].astype(jnp.float32)
                low = base + (x * plan.ny + y) * plan.nz
                parts.append(loaded[name][low : low + plan.nz])
            if plan.high > plan.depth:
                parts.append(jnp.zeros((plan.high - plan.depth, plan.width), jnp.float32))
            columns.append(jnp.concatenate(parts, axis=0))
    return columns


def pick(column, index):
    high = column.shape[0]
    numbers = lax.GatherDimensionNumbers(
        offset_dims=(),
        collapsed_slice_dims=(0,),
        start_index_map=(0,),
        operand_batching_dims=(1,),
        start_indices_batching_dims=(1,),
    )
    found = None
    for group in range(high // 8):
        part = lax.gather(
            column[8 * group : 8 * group + 8],
            (index if high == 8 else index & 7)[..., None],
            numbers,
            (1, 1),
            mode=lax.GatherScatterMode.PROMISE_IN_BOUNDS,
        )
        found = part if found is None else jnp.where(index >> 3 == group, part, found)
    return found


def tables(plan, columns, plane_ref, keep_ref, slots_ref, flags_ref, index_ref, mask_ref):
    for first in range(0, plan.targets, LANES):
        part = jnp.broadcast_to(keep_ref[:, first : first + LANES], (LANES, LANES))
        flags_ref[first : first + LANES, :] = part.T
    line = lax.broadcasted_iota(jnp.int32, (plan.high, LANES), 0).astype(jnp.float32)
    inverses = []
    for number, column in enumerate(columns):
        slots_ref[number] = column
        inverse = jnp.zeros((plan.high, LANES), jnp.int32)
        for slot in range(plan.depth):
            inverse = jnp.where(slots_ref[number, slot : slot + 1, :] == line, slot, inverse)
        inverses.append(inverse)
    step = lax.broadcasted_iota(jnp.int32, (8, LANES), 0).astype(jnp.float32) - 1.0
    for place, (row, i, j) in enumerate(plan.picks):
        x, y, _ = plan.place(row)
        want = plane_ref[row : row + 1, :] + step
        inside = (want >= 0.0) & (want < plan.depth) & (step < 2.0)
        want = jnp.clip(want, 0.0, plan.depth - 1.0).astype(jnp.int32)
        at = row * PITCH + 9 * i + 3 * j
        mask = jnp.where(inside, flags_ref[at : at + 8, :], 0.0)
        _, _, on_grid = plan.beside(x + i, plan.nx, "gx", plan.gx)
        if on_grid is not None:
            mask = jnp.where(on_grid, mask, 0.0)
        if not plan.few:
            _, _, on_grid = plan.beside(y + j, plan.ny, "gy", plan.gy)
            if on_grid is not None:
                mask = jnp.where(on_grid, mask, 0.0)
        at = 8 * place
        index_ref[at : at + 8, :] = pick(inverses[plan.column(row, i, j)], want)
        mask_ref[at : at + 8, :] = mask


def block_of(plan, blocks_ref, row, number):
    x, y, s = plan.place(row)
    i, j, k = plan.entries[number]
    return blocks_ref[x, y, s, 9 * i + 3 * (j + plan.first_span()) + k]


def tile_of(plan, block, row, group, tile_ref):
    size = plan.width
    for quad in group:
        for part in range(4):
            number = 4 * quad + part
            line = size * (2 * quad + part % 2)
            lane = size * (part // 2)
            if number < len(plan.entries):
                values = block(row, number).astype(jnp.float32).T.astype(jnp.bfloat16)
            else:
                values = jnp.zeros((size, size), jnp.bfloat16)
            tile_ref[row, line : line + size, lane : lane + size] = values


def lane_sums(total, multiplied):
    size = total.shape[0]
    if multiplied:
        high = total.astype(jnp.bfloat16)
        low = (total - high.astype(jnp.float32)).astype(jnp.bfloat16)
        sums = lax.dot_general(
            jnp.ones((8, 2 * size), jnp.bfloat16),
            jnp.concatenate([high, low], axis=1),
            (((1,), (1,)), ((), ())),
            preferred_element_type=jnp.float32,
        )
        return sums[:1]
    lane = lax.broadcasted_iota(jnp.int32, (size, size), 1)
    line = lax.broadcasted_iota(jnp.int32, (size, size), 0)
    sums = jnp.sum(total, axis=1, keepdims=True)
    return jnp.sum(jnp.where(lane == line, sums, 0.0), axis=0, keepdims=True)


def product(plan, blocks_ref, tile_ref, wide_ref, received_ref, index_ref, mask_ref, gather_ref, opening=False):
    columns = gathered_columns(plan, received_ref, 0)
    for place, (row, i, j) in enumerate(plan.picks):
        here = slice(8 * place, 8 * place + 8)
        values = pick(columns[plan.column(row, i, j)], index_ref[here, :])
        gather_ref[here, :] = values * mask_ref[here, :]
    size = plan.width
    count = len(plan.entries)
    block = functools.partial(block_of, plan, blocks_ref)

    def pair(row, number):
        blank = jnp.zeros((size, size), jnp.bfloat16)
        sides = [block(row, at) if at < count else blank for at in (number, number + 1)]
        return jnp.concatenate(sides, axis=1)

    def vectors(row, number):
        if number >= count:
            return jnp.zeros((1, size), jnp.float32)
        at = plan.spot(row, number)
        return gather_ref[at : at + 1, :]

    results = []
    for row in plan.tiled:
        found = jnp.zeros((1, size), jnp.float32)
        whole = [quad for quad in range(plan.quads) if 4 * quad + 2 < count]
        cut = len(whole) // 2
        for group in (whole[:cut], whole[cut:], [plan.quads - 1] if plan.quads > len(whole) else []):
            if not group:
                continue
            if opening:
                tile_of(plan, block, row, group, tile_ref)
            left, right = [], []
            for quad in group:
                for side in (0, 1):
                    lines = [vectors(row, 4 * quad + side), vectors(row, 4 * quad + 2 + side)]
                    left.append(jnp.concatenate(lines, axis=0).astype(jnp.bfloat16))
                if opening:
                    parts = [pair(row, at) for at in (4 * quad, 4 * quad + 2) if at < count]
                    right.append(jnp.concatenate(parts, axis=0))
            left = jnp.concatenate(left, axis=1)
            if opening:
                both = lax.dot_general(
                    left,
                    jnp.concatenate(right, axis=1),
                    (((1,), (1,)), ((), ())),
                    preferred_element_type=jnp.float32,
                )
            else:
                here = slice(2 * size * group[0], 2 * size * (group[-1] + 1))
                both = jnp.dot(left, tile_ref[row, here, :], preferred_element_type=jnp.float32)
            found = found + both[:1, :size]
            if both.shape[1] > size:
                found = found + both[1:2, size:]
        results.append(found)
    for place, row in enumerate(plan.plain):
        total = jnp.zeros((size, size), jnp.float32)
        for number in range(count):
            if opening:
                values = block(row, number).astype(jnp.float32)
                wide_ref[place, number] = values
            else:
                values = wide_ref[place, number]
            total = total + values * vectors(row, number)
        results.append(lane_sums(total, opening or row != plan.plain[-1]))
    return jnp.concatenate(results, axis=0)


def opening_kernel(
    plan, received_ref, blocks_ref, plane_ref, keep_ref, start_ref, rhs_ref,
    pay_ref, index_ref, mask_ref, tile_ref, wide_ref, smoothed_ref, remainder_ref, search_ref,
    gather_ref, slots_ref, flags_ref,
):
    columns = gathered_columns(plan, received_ref, plan.rows)
    tables(plan, columns, plane_ref, keep_ref, slots_ref, flags_ref, index_ref, mask_ref)
    remainder = rhs_ref[...] - product(
        plan, blocks_ref, tile_ref, wide_ref, received_ref, index_ref, mask_ref, gather_ref, True
    )
    search = remainder / CENTER
    send(search, pay_ref)
    remainder_ref[...] = remainder
    search_ref[...] = search
    smoothed_ref[...] = start_ref[...] + search


def turn_kernel(
    plan, factors, received_ref, tile_ref, wide_ref, index_ref, mask_ref,
    smoothed_in, remainder_in, search_in,
    pay_ref, smoothed_ref, remainder_ref, *rest,
):
    *search_ref, gather_ref = rest
    remainder = remainder_in[...] - product(
        plan, None, tile_ref, wide_ref, received_ref, index_ref, mask_ref, gather_ref
    )
    search = factors[0] * search_in[...] + factors[1] * remainder
    send(search, pay_ref)
    remainder_ref[...] = remainder
    smoothed_ref[...] = smoothed_in[...] + search
    if search_ref:
        search_ref[0][...] = search


def closing_kernel(
    plan, received_ref, tile_ref, wide_ref, index_ref, mask_ref, smoothed_in, remainder_in,
    smoothed_ref, remainder_ref, gather_ref,
):
    smoothed_ref[...] = smoothed_in[...]
    remainder_ref[...] = remainder_in[...] - product(
        plan, None, tile_ref, wide_ref, received_ref, index_ref, mask_ref, gather_ref
    )


def local(blocks, pattern, order, start, rhs):
    plan = Plan([lax.axis_size(axis) for axis in ("gx", "gy", "gz")], start.shape)
    width = plan.width

    def like(kind, *shape):
        return jax.ShapeDtypeStruct(shape, kind)

    def pay(rows):
        return like(jnp.bfloat16, plan.devices, rows, width)

    state = like(jnp.float32, plan.rows, width)
    scratch = [pltpu.VMEM((8 * len(plan.picks), width), jnp.float32)]

    def call(kernel, ins, outs, scratch_shapes, cost=None):
        return pl.pallas_call(
            kernel,
            in_specs=ins,
            out_specs=[VMEM] * len(outs),
            out_shape=outs,
            scratch_shapes=scratch_shapes,
            compiler_params=pltpu.CompilerParams(vmem_limit_bytes=GRANT),
            cost_estimate=cost,
        )

    def exchange(sent):
        return lax.all_to_all(sent, AXES, 0, 0, tiled=True)

    flat_start = start.reshape(state.shape)
    flat_rhs = rhs.reshape(state.shape)
    sent, plane, keep = call(
        functools.partial(first_kernel, plan),
        [HBM, HBM, HBM],
        [pay(2 * plan.rows), state, like(jnp.float32, 1, plan.targets)],
        [
            pltpu.VMEM(state.shape, jnp.float32),
            pltpu.SMEM(order.shape, jnp.int32),
            pltpu.VMEM(pattern.shape, jnp.int32),
            pltpu.SemaphoreType.DMA((3,)),
        ],
        pl.CostEstimate(flops=10**10, bytes_accessed=10**8, transcendentals=0),
    )(far(order), far(pattern), far(flat_start))
    sent, index, mask, tile, wide, smoothed, remainder, *search = call(
        functools.partial(opening_kernel, plan),
        [VMEM] * 6,
        [
            pay(plan.rows),
            like(jnp.int32, 8 * len(plan.picks), LANES),
            like(jnp.float32, 8 * len(plan.picks), LANES),
            like(jnp.bfloat16, len(plan.tiled), 2 * width * plan.quads, 2 * width),
            like(jnp.float32, len(plan.plain), len(plan.entries), width, width),
            state,
            state,
            state,
        ],
        scratch
        + [
            pltpu.VMEM((plan.columns, plan.high, LANES), jnp.float32),
            pltpu.VMEM((plan.targets, LANES), jnp.float32),
        ],
    )(exchange(sent), blocks, plane, keep, flat_start, flat_rhs)
    sigma = CENTER / SPREAD
    rho = 1.0 / sigma
    for number in range(DEG - 1):
        following = 1.0 / (2.0 * sigma - rho)
        factors = (following * rho, 2.0 * following / SPREAD)
        rho = following
        states = [state] * (3 if number + 2 < DEG else 2)
        sent, smoothed, remainder, *search = call(
            functools.partial(turn_kernel, plan, factors),
            [VMEM] * 8,
            [pay(plan.rows)] + states,
            scratch,
        )(exchange(sent), tile, wide, index, mask, smoothed, remainder, *search)
    smoothed, remainder = call(
        functools.partial(closing_kernel, plan), [VMEM] * 7, [state, state], scratch
    )(exchange(sent), tile, wide, index, mask, smoothed, remainder)
    return smoothed.reshape(start.shape), remainder.reshape(start.shape)


def solution(mesh):
    in_specs = (
        P("gx", "gy", "gz", None, None, None),
        P("gx", "gy", None, None),
        P("gx", "gy", None),
        P("gx", "gy", "gz", None),
        P("gx", "gy", "gz", None),
    )
    out_specs = (P("gx", "gy", "gz", None), P("gx", "gy", "gz", None))
    return jax.shard_map(local, mesh=mesh, in_specs=in_specs, out_specs=out_specs, check_vma=False)
```

```python
import functools

import jax
import jax.numpy as jnp
from jax import lax
from jax.experimental import pallas as pl
from jax.experimental.pallas import tpu as pltpu
from jax.sharding import PartitionSpec as P

DEG = 4
CENTER = 1.0
SPREAD = 0.8
LANES = 128
PITCH = 32
GRANT = 16 * 2**20
AXES = ("gz", "gx", "gy")
VMEM = pl.BlockSpec(memory_space=pltpu.VMEM)
HBM = pl.BlockSpec(memory_space=pltpu.HBM)


def far(array):
    return pltpu.with_memory_space_constraint(array, pltpu.HBM)


class Plan:
    def __init__(self, axis_sizes, local_shape):
        self.gx, self.gy, self.gz = axis_sizes
        self.nx, self.ny, self.nz, self.width = local_shape
        self.devices = self.gx * self.gy * self.gz
        self.rows = self.nx * self.ny * self.nz
        self.sources = self.devices * self.rows
        self.few = self.ny == 1 and self.gy <= 2
        self.spans = min(3, self.gy) if self.few else 3
        self.entries = [(i, j, k) for i in range(3) for j in range(self.spans) for k in range(3)]
        self.targets = -(-self.rows * PITCH // LANES) * LANES
        self.tiled = list(range(self.rows // 4))
        self.plain = list(range(self.rows // 4, self.rows))
        self.quads = -(-len(self.entries) // 4)
        self.depth = self.gz * self.nz
        self.high = -(-self.depth // 8) * 8
        self.across = self.spans if self.few else self.ny + 2
        self.columns = (self.nx + 2) * self.across
        self.picks = [
            (row, i, j) for row in range(self.rows) for i in range(3) for j in range(self.spans)
        ]

    def first_span(self):
        return 1 - lax.axis_index("gy") if self.few else 0

    def place(self, row):
        return row // (self.ny * self.nz), row // self.nz % self.ny, row % self.nz

    def spot(self, row, number):
        i, j, k = self.entries[number]
        return 8 * ((row * 3 + i) * self.spans + j) + k

    def column(self, row, i, j):
        x, y, _ = self.place(row)
        return (x + i) * self.across + (j if self.few else y + j)

    def beside(self, number, count, axis, devices):
        me = lax.axis_index(axis)
        if number == 0:
            return jnp.maximum(me - 1, 0), count - 1, me > 0
        if number == count + 1:
            return jnp.minimum(me + 1, devices - 1), 0, me < devices - 1
        return me, number - 1, None


def send(tile, pay_ref):
    pay_ref[...] = jnp.broadcast_to(tile.astype(jnp.bfloat16)[None], pay_ref.shape)


def first_kernel(
    plan, order_hbm, pattern_hbm, start_hbm,
    pay_ref, plane_ref, keep_ref, start_ref, order_ref, pattern_ref, sems,
):
    copies = (
        pltpu.make_async_copy(order_hbm, order_ref, sems.at[0]),
        pltpu.make_async_copy(pattern_hbm, pattern_ref, sems.at[1]),
        pltpu.make_async_copy(start_hbm, start_ref, sems.at[2]),
    )
    for copy in (copies[1], copies[0], copies[2]):
        copy.start()
    copies[1].wait()
    keep_ref[...] = kept(plan, pattern_ref)
    copies[0].wait()
    copies[2].wait()
    first = lax.axis_index("gz") * plan.nz
    line = lax.broadcasted_iota(jnp.int32, (plan.rows, plan.width), 0)
    planes = jnp.zeros_like(line)
    for row in range(plan.rows):
        x, y, s = plan.place(row)
        planes = jnp.where(line == row, order_ref[x, y, first + s], planes)
    planes = planes.astype(jnp.float32)
    send(jnp.concatenate([start_ref[...], planes], axis=0), pay_ref)
    plane_ref[...] = planes


def kept(plan, pattern_ref):
    first = lax.axis_index("gz") * plan.nz
    span = plan.first_span()
    lane = lax.broadcasted_iota(jnp.int32, (1, plan.targets), 1)
    flat = jnp.zeros_like(lane)
    for number in range(plan.rows):
        x, y, s = plan.place(number)
        flags = pattern_ref[x, y, pl.ds(first + s, 1), :]
        gap = jnp.zeros((1, plan.targets - flags.shape[1]), jnp.int32)
        flags = jnp.concatenate([flags, gap], axis=1)
        turn = lax.rem(plan.targets + PITCH * number - 3 * span, plan.targets)
        flat = flat + pltpu.roll(flags, turn, 1)
    centre = (lane & (PITCH - 1)) + 3 * span == 13
    return jnp.where((flat > 0) | centre, 1.0, 0.0)


def gathered_columns(plan, received_ref, base):
    loaded = {}
    columns = []
    for i in range(plan.nx + 2):
        device_x, x, _ = plan.beside(i, plan.nx, "gx", plan.gx)
        side = (i > 0) + (i > plan.nx)
        for j in range(plan.across):
            if plan.few:
                device_y, y, slice_y = j, 0, j
            else:
                device_y, y, _ = plan.beside(j, plan.ny, "gy", plan.gy)
                slice_y = (j > 0) + (j > plan.ny)
            parts = []
            for z in range(plan.gz):
                name = (side, slice_y, z)
                if name not in loaded:
                    device = (z * plan.gx + device_x) * plan.gy + device_y
                    loaded[name] = received_ref[device].astype(jnp.float32)
                low = base + (x * plan.ny + y) * plan.nz
                parts.append(loaded[name][low : low + plan.nz])
            if plan.high > plan.depth:
                parts.append(jnp.zeros((plan.high - plan.depth, plan.width), jnp.float32))
            columns.append(jnp.concatenate(parts, axis=0))
    return columns


def pick(column, index):
    high = column.shape[0]
    numbers = lax.GatherDimensionNumbers(
        offset_dims=(),
        collapsed_slice_dims=(0,),
        start_index_map=(0,),
        operand_batching_dims=(1,),
        start_indices_batching_dims=(1,),
    )
    found = None
    for group in range(high // 8):
        part = lax.gather(
            column[8 * group : 8 * group + 8],
            (index if high == 8 else index & 7)[..., None],
            numbers,
            (1, 1),
            mode=lax.GatherScatterMode.PROMISE_IN_BOUNDS,
        )
        found = part if found is None else jnp.where(index >> 3 == group, part, found)
    return found


def tables(plan, columns, plane_ref, keep_ref, slots_ref, flags_ref, index_ref, mask_ref):
    for first in range(0, plan.targets, LANES):
        part = jnp.broadcast_to(keep_ref[:, first : first + LANES], (LANES, LANES))
        flags_ref[first : first + LANES, :] = part.T
    line = lax.broadcasted_iota(jnp.int32, (plan.high, LANES), 0).astype(jnp.float32)
    inverses = []
    for number, column in enumerate(columns):
        slots_ref[number] = column
        inverse = jnp.zeros((plan.high, LANES), jnp.int32)
        for slot in range(plan.depth):
            inverse = jnp.where(slots_ref[number, slot : slot + 1, :] == line, slot, inverse)
        inverses.append(inverse)
    step = lax.broadcasted_iota(jnp.int32, (8, LANES), 0).astype(jnp.float32) - 1.0
    for place, (row, i, j) in enumerate(plan.picks):
        x, y, _ = plan.place(row)
        want = plane_ref[row : row + 1, :] + step
        inside = (want >= 0.0) & (want < plan.depth) & (step < 2.0)
        want = jnp.clip(want, 0.0, plan.depth - 1.0).astype(jnp.int32)
        at = row * PITCH + 9 * i + 3 * j
        mask = jnp.where(inside, flags_ref[at : at + 8, :], 0.0)
        _, _, on_grid = plan.beside(x + i, plan.nx, "gx", plan.gx)
        if on_grid is not None:
            mask = jnp.where(on_grid, mask, 0.0)
        if not plan.few:
            _, _, on_grid = plan.beside(y + j, plan.ny, "gy", plan.gy)
            if on_grid is not None:
                mask = jnp.where(on_grid, mask, 0.0)
        at = 8 * place
        index_ref[at : at + 8, :] = pick(inverses[plan.column(row, i, j)], want)
        mask_ref[at : at + 8, :] = mask


def block_of(plan, blocks_ref, row, number):
    x, y, s = plan.place(row)
    i, j, k = plan.entries[number]
    return blocks_ref[x, y, s, 9 * i + 3 * (j + plan.first_span()) + k]


def tile_of(plan, block, row, group, tile_ref):
    size = plan.width
    for quad in group:
        for part in range(4):
            number = 4 * quad + part
            line = size * (2 * quad + part % 2)
            lane = size * (part // 2)
            if number < len(plan.entries):
                values = block(row, number).astype(jnp.float32).T.astype(jnp.bfloat16)
            else:
                values = jnp.zeros((size, size), jnp.bfloat16)
            tile_ref[row, line : line + size, lane : lane + size] = values


def lane_sums(total, multiplied):
    size = total.shape[0]
    if multiplied:
        high = total.astype(jnp.bfloat16)
        low = (total - high.astype(jnp.float32)).astype(jnp.bfloat16)
        sums = lax.dot_general(
            jnp.ones((8, 2 * size), jnp.bfloat16),
            jnp.concatenate([high, low], axis=1),
            (((1,), (1,)), ((), ())),
            preferred_element_type=jnp.float32,
        )
        return sums[:1]
    lane = lax.broadcasted_iota(jnp.int32, (size, size), 1)
    line = lax.broadcasted_iota(jnp.int32, (size, size), 0)
    sums = jnp.sum(total, axis=1, keepdims=True)
    return jnp.sum(jnp.where(lane == line, sums, 0.0), axis=0, keepdims=True)


def product(plan, blocks_ref, tile_ref, wide_ref, received_ref, index_ref, mask_ref, gather_ref, opening=False):
    columns = gathered_columns(plan, received_ref, 0)
    for place, (row, i, j) in enumerate(plan.picks):
        here = slice(8 * place, 8 * place + 8)
        values = pick(columns[plan.column(row, i, j)], index_ref[here, :])
        gather_ref[here, :] = values * mask_ref[here, :]
    size = plan.width
    count = len(plan.entries)
    block = functools.partial(block_of, plan, blocks_ref)

    def pair(row, number):
        blank = jnp.zeros((size, size), jnp.bfloat16)
        sides = [block(row, at) if at < count else blank for at in (number, number + 1)]
        return jnp.concatenate(sides, axis=1)

    def vectors(row, number):
        if number >= count:
            return jnp.zeros((1, size), jnp.float32)
        at = plan.spot(row, number)
        return gather_ref[at : at + 1, :]

    results = []
    for row in plan.tiled:
        found = jnp.zeros((1, size), jnp.float32)
        whole = [quad for quad in range(plan.quads) if 4 * quad + 2 < count]
        cut = len(whole) // 2
        for group in (whole[:cut], whole[cut:], [plan.quads - 1] if plan.quads > len(whole) else []):
            if not group:
                continue
            left, right = [], []
            for quad in group:
                for side in (0, 1):
                    lines = [vectors(row, 4 * quad + side), vectors(row, 4 * quad + 2 + side)]
                    left.append(jnp.concatenate(lines, axis=0).astype(jnp.bfloat16))
                if opening:
                    parts = [pair(row, at) for at in (4 * quad, 4 * quad + 2) if at < count]
                    right.append(jnp.concatenate(parts, axis=0))
            left = jnp.concatenate(left, axis=1)
            if opening:
                both = lax.dot_general(
                    left,
                    jnp.concatenate(right, axis=1),
                    (((1,), (1,)), ((), ())),
                    preferred_element_type=jnp.float32,
                )
            else:
                here = slice(2 * size * group[0], 2 * size * (group[-1] + 1))
                both = jnp.dot(left, tile_ref[row, here, :], preferred_element_type=jnp.float32)
            found = found + both[:1, :size]
            if both.shape[1] > size:
                found = found + both[1:2, size:]
        results.append(found)
    for place, row in enumerate(plan.plain):
        total = jnp.zeros((size, size), jnp.float32)
        for number in range(count):
            if opening:
                values = block(row, number).astype(jnp.float32)
                wide_ref[place, number] = values
            else:
                values = wide_ref[place, number]
            total = total + values * vectors(row, number)
        results.append(lane_sums(total, opening or row != plan.plain[-1]))
    if opening:
        for row in plan.tiled:
            tile_of(plan, block, row, range(plan.quads), tile_ref)
    return jnp.concatenate(results, axis=0)


def opening_kernel(
    plan, received_ref, blocks_ref, plane_ref, keep_ref, start_ref, rhs_ref,
    pay_ref, index_ref, mask_ref, tile_ref, wide_ref, smoothed_ref, remainder_ref, search_ref,
    gather_ref, slots_ref, flags_ref,
):
    columns = gathered_columns(plan, received_ref, plan.rows)
    tables(plan, columns, plane_ref, keep_ref, slots_ref, flags_ref, index_ref, mask_ref)
    remainder = rhs_ref[...] - product(
        plan, blocks_ref, tile_ref, wide_ref, received_ref, index_ref, mask_ref, gather_ref, True
    )
    search = remainder / CENTER
    send(search, pay_ref)
    remainder_ref[...] = remainder
    search_ref[...] = search
    smoothed_ref[...] = start_ref[...] + search


def turn_kernel(
    plan, factors, received_ref, tile_ref, wide_ref, index_ref, mask_ref,
    smoothed_in, remainder_in, search_in,
    pay_ref, smoothed_ref, remainder_ref, *rest,
):
    *search_ref, gather_ref = rest
    remainder = remainder_in[...] - product(
        plan, None, tile_ref, wide_ref, received_ref, index_ref, mask_ref, gather_ref
    )
    search = factors[0] * search_in[...] + factors[1] * remainder
    send(search, pay_ref)
    remainder_ref[...] = remainder
    smoothed_ref[...] = smoothed_in[...] + search
    if search_ref:
        search_ref[0][...] = search


def closing_kernel(
    plan, received_ref, tile_ref, wide_ref, index_ref, mask_ref, smoothed_in, remainder_in,
    smoothed_ref, remainder_ref, gather_ref,
):
    smoothed_ref[...] = smoothed_in[...]
    remainder_ref[...] = remainder_in[...] - product(
        plan, None, tile_ref, wide_ref, received_ref, index_ref, mask_ref, gather_ref
    )


def local(blocks, pattern, order, start, rhs):
    plan = Plan([lax.axis_size(axis) for axis in ("gx", "gy", "gz")], start.shape)
    width = plan.width

    def like(kind, *shape):
        return jax.ShapeDtypeStruct(shape, kind)

    def pay(rows):
        return like(jnp.bfloat16, plan.devices, rows, width)

    state = like(jnp.float32, plan.rows, width)
    scratch = [pltpu.VMEM((8 * len(plan.picks), width), jnp.float32)]

    def call(kernel, ins, outs, scratch_shapes, cost=None):
        return pl.pallas_call(
            kernel,
            in_specs=ins,
            out_specs=[VMEM] * len(outs),
            out_shape=outs,
            scratch_shapes=scratch_shapes,
            compiler_params=pltpu.CompilerParams(vmem_limit_bytes=GRANT),
            cost_estimate=cost,
        )

    def exchange(sent):
        return lax.all_to_all(sent, AXES, 0, 0, tiled=True)

    flat_start = start.reshape(state.shape)
    flat_rhs = rhs.reshape(state.shape)
    sent, plane, keep = call(
        functools.partial(first_kernel, plan),
        [HBM, HBM, HBM],
        [pay(2 * plan.rows), state, like(jnp.float32, 1, plan.targets)],
        [
            pltpu.VMEM(state.shape, jnp.float32),
            pltpu.SMEM(order.shape, jnp.int32),
            pltpu.VMEM(pattern.shape, jnp.int32),
            pltpu.SemaphoreType.DMA((3,)),
        ],
        pl.CostEstimate(flops=10**10, bytes_accessed=10**8, transcendentals=0),
    )(far(order), far(pattern), far(flat_start))
    sent, index, mask, tile, wide, smoothed, remainder, *search = call(
        functools.partial(opening_kernel, plan),
        [VMEM] * 6,
        [
            pay(plan.rows),
            like(jnp.int32, 8 * len(plan.picks), LANES),
            like(jnp.float32, 8 * len(plan.picks), LANES),
            like(jnp.bfloat16, len(plan.tiled), 2 * width * plan.quads, 2 * width),
            like(jnp.float32, len(plan.plain), len(plan.entries), width, width),
            state,
            state,
            state,
        ],
        scratch
        + [
            pltpu.VMEM((plan.columns, plan.high, LANES), jnp.float32),
            pltpu.VMEM((plan.targets, LANES), jnp.float32),
        ],
    )(exchange(sent), blocks, plane, keep, flat_start, flat_rhs)
    sigma = CENTER / SPREAD
    rho = 1.0 / sigma
    for number in range(DEG - 1):
        following = 1.0 / (2.0 * sigma - rho)
        factors = (following * rho, 2.0 * following / SPREAD)
        rho = following
        states = [state] * (3 if number + 2 < DEG else 2)
        sent, smoothed, remainder, *search = call(
            functools.partial(turn_kernel, plan, factors),
            [VMEM] * 8,
            [pay(plan.rows)] + states,
            scratch,
        )(exchange(sent), tile, wide, index, mask, smoothed, remainder, *search)
    smoothed, remainder = call(
        functools.partial(closing_kernel, plan), [VMEM] * 7, [state, state], scratch
    )(exchange(sent), tile, wide, index, mask, smoothed, remainder)
    return smoothed.reshape(start.shape), remainder.reshape(start.shape)


def solution(mesh):
    in_specs = (
        P("gx", "gy", "gz", None, None, None),
        P("gx", "gy", None, None),
        P("gx", "gy", None),
        P("gx", "gy", "gz", None),
        P("gx", "gy", "gz", None),
    )
    out_specs = (P("gx", "gy", "gz", None), P("gx", "gy", "gz", None))
    return jax.shard_map(local, mesh=mesh, in_specs=in_specs, out_specs=out_specs, check_vma=False)
```
